32 devices in a mesh: dom: 32 (over z, y, x, core).
Axes of the slice: x: 2, y: 2, z: 4, core: 2. Of those that a mesh axis runs over, the one named last changes fastest.
Arguments:
- concentration: float32 [1024, 128], P('dom'), may hold values from 0 to 1
- reaction_rate: float32 [1024, 128], P('dom'), may hold values from 0.5 to 4
- step_size: float32 [1], replicated, may hold values from 1 to 2
- block_values: float32 [1024, 5, 128, 128], P('dom'), may hold values from -40 to 48, as said below
- block_columns: int32 [1024, 5], P('dom'), may hold values from 0 to 95, as said below
- row_lengths: int32 [1024], P('dom'), may hold values from 2 to 5, as said below
- send_lists: int32 [32, 4, 16], P('dom'), may hold values from 0 to 31, as said below
Outputs:
- next_concentration: float32 [1024, 128], P('dom')
The draws below stay inside these ranges and needn't reach their ends.
Inputs may be any that keep to these rules, and one draw needn't show every extreme that they name: `send_lists`: for every partition and offset index q (offsets -2, -1, +1, +2), 16 distinct local block indices. `block_columns`: slot 0 of a block row is the row's own local block; live slots name a local block (below 32) or a ghost slot 32 + q * 16 + g of a block that the partition at offset index q sends; slot 1 of local block row q, for q = 0..3, is a ghost slot of offset index q; slots at or past the row's length repeat the row's own local block. `row_lengths`: some block row has all 5 slots live. `block_values`: slot 0 of every block row holds 8 times the identity plus a full random block; the other slots hold full random blocks.
All inputs are finite; a program needn't handle non-finite values.
Results may differ from the reference program's by a relative error of at most 0.00016.
Values sent between devices are 32-bit elements; how exact they have to be, the bound alone decides.
A program may use at most 64 MiB of HBM per device.

```python
import math
import jax
import jax.numpy as jnp
from jax import lax

BLK = 128
BDEV = 32
NNZB = 5
GMAX = 16
KRYLOV = 3
RESTARTS = 2
NDEV = 32
NB = 1024


def ghost_counts(key):
    first_key, second_key = jax.random.split(jax.random.fold_in(key, 11))
    counts = jax.random.randint(first_key, (NDEV, 4), max(GMAX // 4, 1), GMAX + 1)
    fullest = jax.random.randint(second_key, (4,), 0, NDEV)
    devices = jnp.arange(NDEV)[:, None]
    return jnp.where(devices == fullest[None, :], GMAX, counts).astype(jnp.int32)


def lengths_drawn(key):
    first_key, second_key = jax.random.split(jax.random.fold_in(key, 23))
    lengths = jax.random.randint(first_key, (NB,), 2, NNZB + 1)
    longest = jax.random.randint(second_key, (), 0, NB)
    return jnp.where(jnp.arange(NB) == longest, NNZB, lengths).astype(jnp.int32)


def draw_row_lengths(key, part):
    return lengths_drawn(key)


def draw_send_lists(key, part):
    scores = jax.random.randint(jax.random.fold_in(key, 37), (NDEV, 4, BDEV), 0, 1 << 20) * BDEV + jnp.arange(BDEV)
    ordering = jnp.argsort(scores, axis=-1)
    return ordering[:, :, :GMAX].astype(jnp.int32)


def draw_block_columns(key, part):
    counts = ghost_counts(key)
    lengths = lengths_drawn(key)
    subkeys = jax.random.split(jax.random.fold_in(key, 53), 4)
    row_ids = jnp.arange(NB)
    device = row_ids // BDEV
    local_row = row_ids % BDEV
    positions = jnp.arange(NNZB)[None, :]
    forced = (positions == 1) & (local_row[:, None] < 4)
    variety = jax.random.randint(subkeys[0], (NB, NNZB), 0, 2)
    variety = jnp.where(forced, 1, variety)
    owned = jax.random.randint(subkeys[1], (NB, NNZB), 0, BDEV)
    within = jax.random.randint(subkeys[2], (NB, NNZB), 0, 4)
    within = jnp.where(forced, jnp.broadcast_to((local_row % 4)[:, None], (NB, NNZB)), within)
    drawn_bits = jax.random.randint(subkeys[3], (NB, NNZB), 0, 1 << 20)
    offsets = jnp.array([-2, -1, 1, 2])
    sender = (device[:, None] - offsets[within]) % NDEV
    ghost_slot = drawn_bits % counts[sender, within]
    ghost = BDEV + within * GMAX + ghost_slot
    picked = jnp.where(variety == 1, ghost, owned)
    picked = jnp.where(positions == 0, local_row[:, None], picked)
    picked = jnp.where(positions < lengths[:, None], picked, local_row[:, None])
    return picked.astype(jnp.int32)


def draw_block_values(key, part):
    first_key = jax.random.fold_in(jax.random.fold_in(key, 71), 0)
    spread = 4.0 / math.sqrt(BLK * NNZB)
    shape = (NB, NNZB, BLK, BLK)
    entries = jax.random.normal(first_key, shape, jnp.float32)
    diagonal = (jnp.arange(NNZB) == 0).astype(jnp.float32)[None, :, None, None] * jnp.eye(BLK, dtype=jnp.float32)[None, None] * 8.0
    return (entries * spread + diagonal).astype(jnp.float32)


def block_scale(own_key, extent, shards, low, high):
    loudness = 1.0
    for dim, blocks in shards:
        draws = jax.random.uniform(jax.random.fold_in(jax.random.fold_in(own_key, 6), dim), (blocks,), jnp.float32, low / len(shards), high / len(shards))
        loudness = loudness * jnp.repeat(jnp.exp(draws), extent[dim] // blocks).reshape((-1,) + (1,) * (len(extent) - 1 - dim))
    return loudness


def setup_inputs(seed: int = 0) -> dict:
    key_of = jax.random.split(jax.random.key(seed), 8)
    return {
        "concentration": jnp.clip(1.0 * jax.random.uniform(key_of[0], (NB, BLK), jnp.float32) ** block_scale(key_of[0], (NB, BLK), ((0, 32),), -0.2, 0.2), 0.0, 1.0),
        "reaction_rate": jnp.clip(jnp.exp(math.log(4.0) - 2.0794415 * jax.random.uniform(key_of[1], (NB, BLK), jnp.float32) ** block_scale(key_of[1], (NB, BLK), ((0, 32),), -0.2, 0.2)), 0.5, 4.0),
        "step_size": jnp.clip(jax.random.uniform(key_of[2], (1,), jnp.float32, 1.0, 2.0), 1.0, 2.0),
        "block_values": draw_block_values(jax.random.fold_in(key_of[7], 71), 0),
        "block_columns": draw_block_columns(jax.random.fold_in(key_of[7], 71), 0),
        "row_lengths": draw_row_lengths(jax.random.fold_in(key_of[7], 71), 0),
        "send_lists": draw_send_lists(jax.random.fold_in(key_of[7], 71), 0),
    }


epsilon = 1e-06
OFFSETS = (-2, -1, 1, 2)

def column_map(block_columns, send_lists):
    device = (jnp.arange(NB, dtype=jnp.int32) // BDEV)[:, None]
    ghost_index = jnp.maximum(block_columns - BDEV, 0)
    neighbour = ghost_index // GMAX
    ghost_slot = ghost_index % GMAX
    offsets = jnp.array(OFFSETS, jnp.int32)
    sender = (device - offsets[neighbour]) % NDEV
    remote = send_lists[sender, neighbour, ghost_slot]
    owned = device * BDEV + block_columns
    return jnp.where(block_columns < BDEV, owned, sender * BDEV + remote).astype(jnp.int32)

def product(block_values, columns, active, field):
    gathered = field[columns] * active[:, :, None]
    return jnp.einsum('bsij,bsj->bi', block_values, gathered, precision=lax.Precision.HIGHEST)

def phi_column(hessenberg, substep):
    order = hessenberg.shape[0]
    augmented = jnp.zeros((order + 1, order + 1), jnp.float32)
    augmented = augmented.at[:order, :order].set(substep * hessenberg).at[0, order].set(1.0)
    reduced = augmented / 64.0
    identity = jnp.eye(order + 1, dtype=jnp.float32)
    series = identity
    for degree in range(12, 0, -1):
        series = identity + jnp.dot(reduced, series, precision=lax.Precision.HIGHEST) / degree
    for square_turn in range(6):
        series = jnp.dot(series, series, precision=lax.Precision.HIGHEST)
    return series[:order, order]

def krylov(start, apply):
    magnitude = jnp.sqrt(jnp.sum(start * start) + epsilon)
    vectors = jnp.zeros((KRYLOV,) + start.shape, jnp.float32).at[0].set(start / magnitude)
    hessenberg = jnp.zeros((KRYLOV, KRYLOV), jnp.float32)
    for column in range(KRYLOV):
        mapped = apply(vectors[column])
        projection = jnp.einsum('kbi,bi->k', vectors, mapped, precision=lax.Precision.HIGHEST)
        mapped = mapped - jnp.einsum('k,kbi->bi', projection, vectors, precision=lax.Precision.HIGHEST)
        hessenberg = hessenberg.at[:, column].set(projection)
        if column + 1 < KRYLOV:
            length = jnp.sqrt(jnp.sum(mapped * mapped) + epsilon)
            hessenberg = hessenberg.at[column + 1, column].set(length)
            vectors = vectors.at[column + 1].set(mapped / length)
    return (magnitude, vectors, hessenberg)

def reference(concentration, reaction_rate, step_size, block_values, block_columns, row_lengths, send_lists):
    columns = column_map(block_columns, send_lists)
    active = (jnp.arange(NNZB, dtype=jnp.int32)[None, :] < row_lengths[:, None]).astype(jnp.float32)
    slope = reaction_rate * (1.0 - 2.0 * concentration)

    def apply(field):
        return slope * field - product(block_values, columns, active, field)
    forcing = reaction_rate * concentration * (1.0 - concentration) - product(block_values, columns, active, concentration)
    substep = step_size[0] / RESTARTS
    increment = jnp.zeros_like(concentration)
    for restart in range(RESTARTS):
        start = forcing if restart == 0 else apply(increment) + forcing
        magnitude, vectors, hessenberg = krylov(start, apply)
        weights = phi_column(hessenberg, substep)
        increment = increment + substep * magnitude * jnp.einsum('k,kbi->bi', weights, vectors, precision=lax.Precision.HIGHEST)
    return concentration + increment
```

```python
import functools

import jax
import jax.numpy as jnp
from jax import lax
from jax.experimental import pallas as pl
from jax.experimental.pallas import tpu as pltpu
from jax.sharding import PartitionSpec as P

KRYLOV = 3
RESTARTS = 2
OFFSETS = (-2, -1, 1, 2)
SHIFT = 8.0
SCALE = 4.0
TILE = 8
EXCHANGES = 7
epsilon = 1e-06


def total(terms):
    result = terms[0]
    for term in terms[1:]:
        result = result + term
    return result


def quadratic(left, gram, right):
    return total(
        [a * total([gram[i][j] * b for j, b in enumerate(right)]) for i, a in enumerate(left)]
    )


def mapped_coefficients(c):
    result = [-SHIFT * c[0]]
    for i in range(1, len(c)):
        result.append(SCALE * c[i - 1] - SHIFT * c[i])
    result.append(SCALE * c[-1])
    return result


def subtract(a, weight, b):
    return [x - weight * b[i] if i < len(b) else x for i, x in enumerate(a)]


def multiply(a, b):
    size = len(a)
    result = []
    for i in range(size):
        row = []
        for j in range(size):
            terms = [
                a[i][k] * b[k][j]
                for k in range(size)
                if a[i][k] is not None and b[k][j] is not None
            ]
            row.append(total(terms) if terms else None)
        result.append(row)
    return result


def plus_identity(a, weight):
    return [
        [x * weight + 1.0 if i == j else x * weight for j, x in enumerate(row)]
        for i, row in enumerate(a)
    ]


def phi_column(hessenberg, substep):
    size = len(hessenberg)
    x = [
        [None if h is None else substep * h * (1.0 / 64.0) for h in row] for row in hessenberg
    ]
    one = jnp.ones_like(substep)
    zero = jnp.zeros_like(substep)
    series = [[one if i == j else zero for j in range(size)] for i in range(size)]
    for degree in range(12, 1, -1):
        series = plus_identity(multiply(x, series), 1.0 / degree)
    column = [series[i][0] * (1.0 / 64.0) for i in range(size)]
    power = plus_identity(multiply(x, series), 1.0)
    for turn in range(6):
        column = [
            total([power[i][k] * column[k] for k in range(size)]) + column[i] for i in range(size)
        ]
        if turn < 5:
            power = multiply(power, power)
    return column


def restart_coefficients(gram, substep):
    magnitude = jnp.sqrt(gram[0][0] + epsilon)
    basis = [[1.0 / magnitude]]
    hessenberg = [[None] * KRYLOV for _ in range(KRYLOV)]
    for column in range(KRYLOV):
        mapped = mapped_coefficients(basis[column])
        residue = mapped
        for k in range(column + 1):
            projection = quadratic(basis[k], gram, mapped)
            hessenberg[k][column] = projection
            residue = subtract(residue, projection, basis[k])
        if column + 1 < KRYLOV:
            squared = jnp.maximum(quadratic(residue, gram, residue), 0.0)
            length = jnp.sqrt(squared + epsilon)
            hessenberg[column + 1][column] = length
            inverse = 1.0 / length
            basis.append([x * inverse for x in residue])
    weights = phi_column(hessenberg, substep)
    factor = substep * magnitude
    return [
        factor * total([weights[k] * basis[k][i] for k in range(i, KRYLOV)]) for i in range(KRYLOV)
    ]


def merge_rows(parts):
    sublane = lax.broadcasted_iota(jnp.int32, parts[0].shape, 0)
    distance = 1
    while len(parts) > 1:
        first = (sublane // distance) % 2 == 0
        parts = [
            jnp.where(first, u, v)
            + pltpu.roll(jnp.where(first, v, u), TILE - distance, 0)
            for u, v in zip(parts[0::2], parts[1::2])
        ]
        distance *= 2
    return parts[0]


def kernel(n, *refs):
    operands, a_ref, y = refs[:6], refs[6], refs[7]
    staged = refs[8:14]
    step_ref, columns_ref, lengths_ref, lists_ref, c_ref, r_ref = staged
    scratch = list(refs[14:])
    stage_sem, inverse, order, table, places, a, local, rates, mixed = scratch[:9]
    scratch = scratch[9:]
    extended = scratch[:EXCHANGES]
    packets = scratch[EXCHANGES : 2 * EXCHANGES]
    rest = scratch[2 * EXCHANGES :]
    sums, partial = rest[:RESTARTS], rest[RESTARTS : 2 * RESTARTS]
    load_sem, send_sem, recv_sem, sum_send, sum_recv = rest[2 * RESTARTS :]

    bdev, width = c_ref.shape
    slots = columns_ref.shape[0]
    sides, gmax = lists_ref.shape
    blank = bdev + sides * gmax
    me = lax.axis_index("dom")

    barrier = pltpu.get_barrier_semaphore()

    def greet(d, carry):
        pl.semaphore_signal(
            barrier,
            inc=1,
            device_id=(lax.rem(me + d, n),),
            device_id_type=pl.DeviceIdType.MESH,
        )
        return carry

    stages = [
        pltpu.make_async_copy(source, target, stage_sem.at[i])
        for i, (source, target) in enumerate(zip(operands, staged))
    ]
    for copy in stages:
        copy.start()
    lax.fori_loop(1, n, greet, 0)
    loads = []
    for g in range(0, bdev, TILE):
        rows = pl.ds(g, TILE)
        copy = pltpu.make_async_copy(a_ref.at[rows], a.at[rows], load_sem.at[g // TILE])
        copy.start()
        loads.append(copy)
    for copy in stages:
        copy.wait()

    lead = (sides - 1) * lax.div(2 * me, n)

    def side(j):
        q = lax.rem(lead + j, sides)
        return q, q - 2 + lax.div(q, 2)

    def remote(e, q, offset, slot, source):
        return pltpu.make_async_remote_copy(
            src_ref=source,
            dst_ref=extended[e].at[pl.ds(bdev + q * gmax, gmax)],
            send_sem=send_sem.at[e, slot],
            recv_sem=recv_sem.at[e, q],
            device_id=(lax.rem(me + offset + n, n),),
            device_id_type=pl.DeviceIdType.MESH,
        )

    def first_copies():
        return [
            remote(0, q, offset, q, packets[0].at[q]) for q, offset in enumerate(OFFSETS)
        ]

    def copy_of(e, j):
        q, offset = side(j)
        source = packets[e].at[j] if j else extended[e].at[pl.ds(0, gmax)]
        return remote(e, q, offset, j, source)

    def send_lead(e):
        copy_of(e, 0).start()

    def send_rest(e):
        for j in range(1, sides):
            q, _ = side(j)
            for g in range(gmax):
                packets[e][j, g : g + 1, :] = local[pl.ds(places[q * gmax + g], 1), :]
        for j in range(1, sides):
            copy_of(e, j).start()

    def arrive(e):
        for q in range(sides):
            remote(e, q, 0, q, extended[e].at[pl.ds(0, gmax)]).wait_recv()

    def clear(target):
        target[blank:, :] = jnp.zeros((8, width), jnp.float32)

    for q in range(sides):
        for g in range(gmax):
            packets[0][q, g : g + 1, :] = c_ref[pl.ds(lists_ref[q, g], 1), :]
    pl.semaphore_wait(barrier, n - 1)
    for copy in first_copies():
        copy.start()

    def fill_inverse(row, carry):
        hit = jnp.int32(0)
        below = jnp.int32(0)
        for i in range(gmax):
            listed = lists_ref[lead, i]
            hit = jnp.where(listed == row, i + 1, hit)
            below = below + jnp.where(listed < row, 1, 0)
        inverse[row] = jnp.where(hit > 0, hit - 1, gmax + row - below)
        return carry

    lax.fori_loop(0, bdev, fill_inverse, 0)

    def fill_lead(i, carry):
        order[i] = lists_ref[lead, i]
        for q in range(sides):
            places[q * gmax + i] = inverse[lists_ref[q, i]]
        return carry

    lax.fori_loop(0, gmax, fill_lead, 0)

    def fill_others(i, carry):
        row = jnp.int32(0)
        for r in range(bdev):
            row = row + jnp.where(inverse[r] == i, r, 0)
        order[i] = row
        return carry

    lax.fori_loop(gmax, bdev, fill_others, 0)

    def fill_table(i, carry):
        row = order[i]
        length = lengths_ref[row]
        for t in range(1, slots):
            column = columns_ref[t, row]
            place = jnp.where(column < bdev, inverse[jnp.minimum(column, bdev - 1)], column)
            table[i * slots + t] = jnp.where(t < length, place, blank)
        return carry

    lax.fori_loop(0, bdev, fill_table, 0)

    def rowsum(products):
        turned = products.T
        return total([turned[k : k + TILE, :] for k in range(0, width, TILE)])

    def own_product(x):
        result = []
        for g in range(0, bdev, TILE):
            result.append(
                merge_rows(
                    [rowsum(a[order[i], 0] * x[i : i + 1, :]) for i in range(g, g + TILE)]
                )
            )
        return jnp.concatenate(result, axis=0)

    def other_product(source, start, stop):
        result = []
        for g in range(start, stop, TILE):
            parts = []
            for i in range(g, g + TILE):
                row = order[i]
                parts.append(
                    rowsum(
                        total(
                            [
                                a[row, t] * source[pl.ds(table[i * slots + t], 1), :]
                                for t in range(1, slots)
                            ]
                        )
                    )
                )
            result.append(merge_rows(parts))
        return jnp.concatenate(result, axis=0)

    lane = lax.broadcasted_iota(jnp.int32, (1, width), 1)

    def dots(row, fields, last):
        for i in range(last + 1):
            folded = jnp.sum(fields[i] * fields[last], axis=0, keepdims=True)
            value = jnp.sum(folded, axis=1, keepdims=True)
            row = jnp.where(lane == last * (last + 1) // 2 + i, value, row)
        return row

    def send_sums(turn, row):
        partial[turn][...] = row
        sums[turn][me] = row

        def one(d, carry):
            pltpu.make_async_remote_copy(
                src_ref=partial[turn],
                dst_ref=sums[turn].at[me],
                send_sem=sum_send.at[turn],
                recv_sem=sum_recv.at[turn],
                device_id=(lax.rem(me + d, n),),
                device_id_type=pl.DeviceIdType.MESH,
            ).start()
            return carry

        lax.fori_loop(1, n, one, 0)

    def gather_sums(turn, count):
        others = sums[turn].at[pl.ds(0, n - 1)]
        pltpu.make_async_copy(others, others, sum_recv.at[turn]).wait()
        row = jnp.sum(sums[turn][...], axis=0)
        gram = [[None] * count for _ in range(count)]
        for j in range(count):
            for i in range(j + 1):
                index = j * (j + 1) // 2 + i
                value = jnp.sum(jnp.where(lane == index, row, 0.0), axis=1, keepdims=True)
                gram[i][j] = gram[j][i] = jnp.broadcast_to(value, (8, width))
        return gram

    def combine(weights, fields):
        return total(
            [
                jnp.concatenate([w] * (f.shape[0] // 8), axis=0) * f
                for w, f in zip(weights, fields)
            ]
        )

    for i in range(bdev):
        row = order[i]
        local[i : i + 1, :] = c_ref[pl.ds(row, 1), :]
        rates[i : i + 1, :] = r_ref[pl.ds(row, 1), :]
    concentration = local[...]
    rate = rates[...]
    shifted = (rate * (1.0 - 2.0 * concentration) + SHIFT) * (1.0 / SCALE)
    substep = jnp.full((8, width), step_ref[0] * (1.0 / RESTARTS), jnp.float32)
    for e in range(EXCHANGES):
        clear(extended[e])
    clear(mixed)

    def finish(e, source, known, scale):
        parts = []
        for start in range(0, bdev, gmax):
            rows = slice(start, start + gmax)
            part = known[rows] - scale * other_product(source, start, start + gmax)
            parts.append(part)
            if e is not None:
                extended[e][rows, :] = part
                local[rows, :] = part
                if start == 0:
                    send_lead(e)
        if e is not None:
            send_rest(e)
        return jnp.concatenate(parts, axis=0)

    def known_part(field):
        return shifted * field - own_product(field) * (1.0 / SCALE)

    extended[0][0:bdev, :] = concentration
    for copy in loads:
        copy.wait()
    known = rate * concentration * (1.0 - concentration) - own_product(concentration)
    arrive(0)
    field = finish(1, extended[0], known, 1.0)

    fields = [field]
    row = jnp.zeros((1, width), jnp.float32)
    for j in range(KRYLOV):
        row = dots(row, fields, j)
        known = known_part(field)
        arrive(1 + j)
        field = finish(2 + j, extended[1 + j], known, 1.0 / SCALE)
        fields.append(field)

    e = KRYLOV + 1
    send_sums(0, dots(row, fields, KRYLOV))
    known = known_part(field)
    arrive(e)
    field = finish(e + 1, extended[e], known, 1.0 / SCALE)
    fields.append(field)
    e = KRYLOV + 2
    d = restart_coefficients(gather_sums(0, KRYLOV + 1), substep)
    s = mapped_coefficients(d)
    s[0] = s[0] + 1.0
    start = combine(s, fields[:-1])
    field = combine(s, fields[1:])
    base = concentration + combine(d, fields[:KRYLOV])
    mixed[0:bdev, :] = field
    known = known_part(field)
    fields = [start, field]
    row = jnp.zeros((1, width), jnp.float32)
    row = dots(dots(row, fields, 0), fields, 1)
    arrive(e)
    mixed[bdev:blank, :] = combine(
        s, [extended[2 + j][bdev:blank, :] for j in range(KRYLOV + 1)]
    )
    source = mixed
    for j in range(2, KRYLOV + 1):
        e = KRYLOV + 1 + j
        field = finish(e if j < KRYLOV else None, source, known, 1.0 / SCALE)
        fields.append(field)
        if j < KRYLOV:
            row = dots(row, fields, j)
            known = known_part(field)
            arrive(e)
            source = extended[e]
    send_sums(1, dots(row, fields, KRYLOV))
    d = restart_coefficients(gather_sums(1, KRYLOV + 1), substep)
    local[...] = base + combine(d, fields[:KRYLOV])
    for r in range(bdev):
        y[r : r + 1, :] = local[pl.ds(inverse[r], 1), :]

    for copy in first_copies():
        copy.wait_send()
    for e in range(1, EXCHANGES):
        for j in range(sides):
            copy_of(e, j).wait_send()
    for turn in range(RESTARTS):
        others = sums[turn].at[pl.ds(0, n - 1)]
        pltpu.make_async_copy(others, others, sum_send.at[turn]).wait()


def solution(mesh):
    n = mesh.shape["dom"]

    def shards(c, r, step, values, columns, lengths, lists):
        bdev, width = c.shape
        slots = columns.shape[1]
        sides, gmax = lists.shape[1:]
        tall = bdev + sides * gmax + 8
        f32 = jnp.float32
        held = pl.BlockSpec(memory_space=pltpu.HBM)
        vmem = pl.BlockSpec(memory_space=pltpu.VMEM)
        return pl.pallas_call(
            functools.partial(kernel, n),
            out_shape=jax.ShapeDtypeStruct((bdev, width), f32),
            in_specs=[held] * 7,
            out_specs=vmem,
            scratch_shapes=[
                pltpu.SMEM((1,), f32),
                pltpu.SMEM((slots, bdev), jnp.int32),
                pltpu.SMEM((bdev,), jnp.int32),
                pltpu.SMEM((sides, gmax), jnp.int32),
                pltpu.VMEM((bdev, width), f32),
                pltpu.VMEM((bdev, width), f32),
                pltpu.SemaphoreType.DMA((6,)),
                pltpu.SMEM((bdev,), jnp.int32),
                pltpu.SMEM((bdev,), jnp.int32),
                pltpu.SMEM((bdev * slots,), jnp.int32),
                pltpu.SMEM((sides * gmax,), jnp.int32),
                pltpu.VMEM((bdev, slots, width, width), f32),
                pltpu.VMEM((bdev, width), f32),
                pltpu.VMEM((bdev, width), f32),
                pltpu.VMEM((tall, width), f32),
            ]
            + [pltpu.VMEM((tall, width), f32)] * EXCHANGES
            + [pltpu.VMEM((sides, gmax, width), f32)] * EXCHANGES
            + [pltpu.VMEM((n, 1, width), f32)] * RESTARTS
            + [pltpu.VMEM((1, width), f32)] * RESTARTS
            + [
                pltpu.SemaphoreType.DMA((bdev // TILE,)),
                pltpu.SemaphoreType.DMA((EXCHANGES, sides)),
                pltpu.SemaphoreType.DMA((EXCHANGES, sides)),
                pltpu.SemaphoreType.DMA((RESTARTS,)),
                pltpu.SemaphoreType.DMA((RESTARTS,)),
            ],
            compiler_params=pltpu.CompilerParams(
                collective_id=0, has_side_effects=True, vmem_limit_bytes=67043328
            ),
        )(step, columns.T, lengths, lists[0], c, r, values)

    placed = (
        P("dom", None),
        P("dom", None),
        P(),
        P("dom", None, None, None),
        P("dom", None),
        P("dom"),
        P("dom", None, None),
    )
    return jax.shard_map(
        shards, mesh=mesh, in_specs=placed, out_specs=P("dom", None), check_vma=False
    )
```

```python
import functools

import jax
import jax.numpy as jnp
from jax import lax
from jax.experimental import pallas as pl
from jax.experimental.pallas import tpu as pltpu
from jax.sharding import PartitionSpec as P

KRYLOV = 3
RESTARTS = 2
OFFSETS = (-2, -1, 1, 2)
SHIFT = 8.0
SCALE = 4.0
TILE = 8
EXCHANGES = 7
epsilon = 1e-06


def total(terms):
    result = terms[0]
    for term in terms[1:]:
        result = result + term
    return result


def quadratic(left, gram, right):
    return total(
        [a * total([gram[i][j] * b for j, b in enumerate(right)]) for i, a in enumerate(left)]
    )


def mapped_coefficients(c):
    result = [-SHIFT * c[0]]
    for i in range(1, len(c)):
        result.append(SCALE * c[i - 1] - SHIFT * c[i])
    result.append(SCALE * c[-1])
    return result


def subtract(a, weight, b):
    return [x - weight * b[i] if i < len(b) else x for i, x in enumerate(a)]


def multiply(a, b):
    size = len(a)
    result = []
    for i in range(size):
        row = []
        for j in range(size):
            terms = [
                a[i][k] * b[k][j]
                for k in range(size)
                if a[i][k] is not None and b[k][j] is not None
            ]
            row.append(total(terms) if terms else None)
        result.append(row)
    return result


def plus_identity(a, weight):
    return [
        [x * weight + 1.0 if i == j else x * weight for j, x in enumerate(row)]
        for i, row in enumerate(a)
    ]


def phi_column(hessenberg, substep):
    size = len(hessenberg)
    x = [
        [None if h is None else substep * h * (1.0 / 64.0) for h in row] for row in hessenberg
    ]
    one = jnp.ones_like(substep)
    zero = jnp.zeros_like(substep)
    series = [[one if i == j else zero for j in range(size)] for i in range(size)]
    for degree in range(12, 1, -1):
        series = plus_identity(multiply(x, series), 1.0 / degree)
    column = [series[i][0] * (1.0 / 64.0) for i in range(size)]
    power = plus_identity(multiply(x, series), 1.0)
    for turn in range(6):
        column = [
            total([power[i][k] * column[k] for k in range(size)]) + column[i] for i in range(size)
        ]
        if turn < 5:
            power = multiply(power, power)
    return column


def restart_coefficients(gram, substep):
    magnitude = jnp.sqrt(gram[0][0] + epsilon)
    basis = [[1.0 / magnitude]]
    hessenberg = [[None] * KRYLOV for _ in range(KRYLOV)]
    for column in range(KRYLOV):
        mapped = mapped_coefficients(basis[column])
        residue = mapped
        for k in range(column + 1):
            projection = quadratic(basis[k], gram, mapped)
            hessenberg[k][column] = projection
            residue = subtract(residue, projection, basis[k])
        if column + 1 < KRYLOV:
            squared = jnp.maximum(quadratic(residue, gram, residue), 0.0)
            length = jnp.sqrt(squared + epsilon)
            hessenberg[column + 1][column] = length
            inverse = 1.0 / length
            basis.append([x * inverse for x in residue])
    weights = phi_column(hessenberg, substep)
    factor = substep * magnitude
    return [
        factor * total([weights[k] * basis[k][i] for k in range(i, KRYLOV)]) for i in range(KRYLOV)
    ]


def merge_rows(parts):
    sublane = lax.broadcasted_iota(jnp.int32, parts[0].shape, 0)
    distance = 1
    while len(parts) > 1:
        first = (sublane // distance) % 2 == 0
        parts = [
            jnp.where(first, u, v)
            + pltpu.roll(jnp.where(first, v, u), TILE - distance, 0)
            for u, v in zip(parts[0::2], parts[1::2])
        ]
        distance *= 2
    return parts[0]


def kernel(n, *refs):
    operands, a_ref, y = refs[:6], refs[6], refs[7]
    staged = refs[8:14]
    step_ref, columns_ref, lengths_ref, lists_ref, c_ref, r_ref = staged
    scratch = list(refs[14:])
    stage_sem, inverse, order, table, places, a, local, rates, mixed = scratch[:9]
    scratch = scratch[9:]
    extended = scratch[:EXCHANGES]
    packets = scratch[EXCHANGES : 2 * EXCHANGES]
    rest = scratch[2 * EXCHANGES :]
    sums, partial = rest[:RESTARTS], rest[RESTARTS : 2 * RESTARTS]
    load_sem, send_sem, recv_sem, sum_send, sum_recv = rest[2 * RESTARTS :]

    bdev, width = c_ref.shape
    slots = columns_ref.shape[0]
    sides, gmax = lists_ref.shape
    blank = bdev + sides * gmax
    me = lax.axis_index("dom")

    barrier = pltpu.get_barrier_semaphore()

    def greet(d, carry):
        pl.semaphore_signal(
            barrier,
            inc=1,
            device_id=(lax.rem(me + d, n),),
            device_id_type=pl.DeviceIdType.MESH,
        )
        return carry

    stages = [
        pltpu.make_async_copy(source, target, stage_sem.at[i])
        for i, (source, target) in enumerate(zip(operands, staged))
    ]
    for copy in stages:
        copy.start()
    lax.fori_loop(1, n, greet, 0)
    loads = []
    for g in range(0, bdev, TILE):
        rows = pl.ds(g, TILE)
        copy = pltpu.make_async_copy(a_ref.at[rows], a.at[rows], load_sem.at[g // TILE])
        copy.start()
        loads.append(copy)
    for copy in stages:
        copy.wait()

    lead = (sides - 1) * lax.div(2 * me, n)

    def side(j):
        q = lax.rem(lead + j, sides)
        return q, q - 2 + lax.div(q, 2)

    def remote(e, q, offset, slot, source):
        return pltpu.make_async_remote_copy(
            src_ref=source,
            dst_ref=extended[e].at[pl.ds(bdev + q * gmax, gmax)],
            send_sem=send_sem.at[e, slot],
            recv_sem=recv_sem.at[e, q],
            device_id=(lax.rem(me + offset + n, n),),
            device_id_type=pl.DeviceIdType.MESH,
        )

    def first_copies():
        return [
            remote(0, q, offset, q, packets[0].at[q]) for q, offset in enumerate(OFFSETS)
        ]

    def copy_of(e, j):
        q, offset = side(j)
        source = packets[e].at[j] if j else extended[e].at[pl.ds(0, gmax)]
        return remote(e, q, offset, j, source)

    def send_lead(e):
        copy_of(e, 0).start()

    def send_rest(e):
        for j in range(1, sides):
            q, _ = side(j)
            for g in range(gmax):
                packets[e][j, g : g + 1, :] = local[pl.ds(places[q * gmax + g], 1), :]
        for j in range(1, sides):
            copy_of(e, j).start()

    def arrive(e):
        for q in range(sides):
            remote(e, q, 0, q, extended[e].at[pl.ds(0, gmax)]).wait_recv()

    def clear(target):
        target[blank:, :] = jnp.zeros((8, width), jnp.float32)

    for q in range(sides):
        for g in range(gmax):
            packets[0][q, g : g + 1, :] = c_ref[pl.ds(lists_ref[q, g], 1), :]
    pl.semaphore_wait(barrier, n - 1)
    for copy in first_copies():
        copy.start()

    def fill_inverse(row, carry):
        hit = jnp.int32(0)
        below = jnp.int32(0)
        for i in range(gmax):
            listed = lists_ref[lead, i]
            hit = jnp.where(listed == row, i + 1, hit)
            below = below + jnp.where(listed < row, 1, 0)
        inverse[row] = jnp.where(hit > 0, hit - 1, gmax + row - below)
        return carry

    lax.fori_loop(0, bdev, fill_inverse, 0)

    def fill_lead(i, carry):
        order[i] = lists_ref[lead, i]
        for q in range(sides):
            places[q * gmax + i] = inverse[lists_ref[q, i]]
        return carry

    lax.fori_loop(0, gmax, fill_lead, 0)

    def fill_others(i, carry):
        row = jnp.int32(0)
        for r in range(bdev):
            row = row + jnp.where(inverse[r] == i, r, 0)
        order[i] = row
        return carry

    lax.fori_loop(gmax, bdev, fill_others, 0)

    def fill_table(i, carry):
        row = order[i]
        length = lengths_ref[row]
        for t in range(1, slots):
            column = columns_ref[t, row]
            place = jnp.where(column < bdev, inverse[jnp.minimum(column, bdev - 1)], column)
            table[i * slots + t] = jnp.where(t < length, place, blank)
        return carry

    lax.fori_loop(0, bdev, fill_table, 0)

    def rowsum(products):
        turned = products.T
        return total([turned[k : k + TILE, :] for k in range(0, width, TILE)])

    def own_product(x):
        result = []
        for g in range(0, bdev, TILE):
            result.append(
                merge_rows(
                    [rowsum(a[order[i], 0] * x[i : i + 1, :]) for i in range(g, g + TILE)]
                )
            )
        return jnp.concatenate(result, axis=0)

    def other_product(source, start, stop):
        result = []
        for g in range(start, stop, TILE):
            parts = []
            for i in range(g, g + TILE):
                row = order[i]
                parts.append(
                    rowsum(
                        total(
                            [
                                a[row, t] * source[pl.ds(table[i * slots + t], 1), :]
                                for t in range(1, slots)
                            ]
                        )
                    )
                )
            result.append(merge_rows(parts))
        return jnp.concatenate(result, axis=0)

    lane = lax.broadcasted_iota(jnp.int32, (1, width), 1)

    def dots(row, fields, last):
        for i in range(last + 1):
            folded = jnp.sum(fields[i] * fields[last], axis=0, keepdims=True)
            value = jnp.sum(folded, axis=1, keepdims=True)
            row = jnp.where(lane == last * (last + 1) // 2 + i, value, row)
        return row

    def send_sums(turn, row):
        partial[turn][...] = row
        sums[turn][me] = row

        def one(d, carry):
            pltpu.make_async_remote_copy(
                src_ref=partial[turn],
                dst_ref=sums[turn].at[me],
                send_sem=sum_send.at[turn],
                recv_sem=sum_recv.at[turn],
                device_id=(lax.rem(me + d, n),),
                device_id_type=pl.DeviceIdType.MESH,
            ).start()
            return carry

        lax.fori_loop(1, n, one, 0)

    def gather_sums(turn, count):
        others = sums[turn].at[pl.ds(0, n - 1)]
        pltpu.make_async_copy(others, others, sum_recv.at[turn]).wait()
        row = jnp.sum(sums[turn][...], axis=0)
        gram = [[None] * count for _ in range(count)]
        for j in range(count):
            for i in range(j + 1):
                index = j * (j + 1) // 2 + i
                value = jnp.sum(jnp.where(lane == index, row, 0.0), axis=1, keepdims=True)
                gram[i][j] = gram[j][i] = jnp.broadcast_to(value, (8, width))
        return gram

    def combine(weights, fields):
        return total(
            [
                jnp.concatenate([w] * (f.shape[0] // 8), axis=0) * f
                for w, f in zip(weights, fields)
            ]
        )

    for i in range(bdev):
        row = order[i]
        local[i : i + 1, :] = c_ref[pl.ds(row, 1), :]
        rates[i : i + 1, :] = r_ref[pl.ds(row, 1), :]
    concentration = local[...]
    rate = rates[...]
    shifted = (rate * (1.0 - 2.0 * concentration) + SHIFT) * (1.0 / SCALE)
    substep = jnp.full((8, width), step_ref[0] * (1.0 / RESTARTS), jnp.float32)
    for e in range(EXCHANGES):
        clear(extended[e])
    clear(mixed)

    def finish(e, source, known, scale):
        parts = []
        for start in range(0, bdev, gmax):
            rows = slice(start, start + gmax)
            part = known[rows] - scale * other_product(source, start, start + gmax)
            parts.append(part)
            if e is not None:
                extended[e][rows, :] = part
                local[rows, :] = part
                if start == 0:
                    send_lead(e)
        if e is not None:
            send_rest(e)
        return jnp.concatenate(parts, axis=0)

    def known_part(field):
        return shifted * field - own_product(field) * (1.0 / SCALE)

    extended[0][0:bdev, :] = concentration
    for copy in loads:
        copy.wait()
    known = rate * concentration * (1.0 - concentration) - own_product(concentration)
    arrive(0)
    field = finish(1, extended[0], known, 1.0)

    fields = [field]
    row = jnp.zeros((1, width), jnp.float32)
    for j in range(KRYLOV):
        row = dots(row, fields, j)
        known = known_part(field)
        arrive(1 + j)
        field = finish(2 + j, extended[1 + j], known, 1.0 / SCALE)
        fields.append(field)

    e = KRYLOV + 1
    send_sums(0, dots(row, fields, KRYLOV))
    known = known_part(field)
    arrive(e)
    field = finish(e + 1, extended[e], known, 1.0 / SCALE)
    fields.append(field)
    e = KRYLOV + 2
    d = restart_coefficients(gather_sums(0, KRYLOV + 1), substep)
    s = mapped_coefficients(d)
    s[0] = s[0] + 1.0
    start = combine(s, fields[:-1])
    field = combine(s, fields[1:])
    base = concentration + combine(d, fields[:KRYLOV])
    mixed[0:bdev, :] = field
    known = known_part(field)
    fields = [start, field]
    row = jnp.zeros((1, width), jnp.float32)
    row = dots(dots(row, fields, 0), fields, 1)
    arrive(e)
    mixed[bdev:blank, :] = combine(
        s, [extended[2 + j][bdev:blank, :] for j in range(KRYLOV + 1)]
    )
    source = mixed
    for j in range(2, KRYLOV + 1):
        e = KRYLOV + 1 + j
        field = finish(e if j < KRYLOV else None, source, known, 1.0 / SCALE)
        fields.append(field)
        if j < KRYLOV:
            row = dots(row, fields, j)
            known = known_part(field)
            arrive(e)
            source = extended[e]
    send_sums(1, dots(row, fields, KRYLOV))
    d = restart_coefficients(gather_sums(1, KRYLOV + 1), substep)
    local[...] = base + combine(d, fields[:KRYLOV])
    for r in range(bdev):
        y[r : r + 1, :] = local[pl.ds(inverse[r], 1), :]

    for copy in first_copies():
        copy.wait_send()
    for e in range(1, EXCHANGES):
        for j in range(sides):
            copy_of(e, j).wait_send()
    for turn in range(RESTARTS):
        others = sums[turn].at[pl.ds(0, n - 1)]
        pltpu.make_async_copy(others, others, sum_send.at[turn]).wait()


def solution(mesh):
    n = mesh.shape["dom"]

    def shards(c, r, step, values, columns, lengths, lists):
        bdev, width = c.shape
        slots = columns.shape[1]
        sides, gmax = lists.shape[1:]
        tall = bdev + sides * gmax + 8
        f32 = jnp.float32
        held = pl.BlockSpec(memory_space=pltpu.HBM)
        vmem = pl.BlockSpec(memory_space=pltpu.VMEM)
        return pl.pallas_call(
            functools.partial(kernel, n),
            out_shape=jax.ShapeDtypeStruct((bdev, width), f32),
            in_specs=[held] * 7,
            out_specs=vmem,
            scratch_shapes=[
                pltpu.SMEM((1,), f32),
                pltpu.SMEM((slots, bdev), jnp.int32),
                pltpu.SMEM((bdev,), jnp.int32),
                pltpu.SMEM((sides, gmax), jnp.int32),
                pltpu.VMEM((bdev, width), f32),
                pltpu.VMEM((bdev, width), f32),
                pltpu.SemaphoreType.DMA((6,)),
                pltpu.SMEM((bdev,), jnp.int32),
                pltpu.SMEM((bdev,), jnp.int32),
                pltpu.SMEM((bdev * slots,), jnp.int32),
                pltpu.SMEM((sides * gmax,), jnp.int32),
                pltpu.VMEM((bdev, slots, width, width), f32),
                pltpu.VMEM((bdev, width), f32),
                pltpu.VMEM((bdev, width), f32),
                pltpu.VMEM((tall, width), f32),
            ]
            + [pltpu.VMEM((tall, width), f32)] * EXCHANGES
            + [pltpu.VMEM((sides, gmax, width), f32)] * EXCHANGES
            + [pltpu.VMEM((n, 1, width), f32)] * RESTARTS
            + [pltpu.VMEM((1, width), f32)] * RESTARTS
            + [
                pltpu.SemaphoreType.DMA((bdev // TILE,)),
                pltpu.SemaphoreType.DMA((EXCHANGES, sides)),
                pltpu.SemaphoreType.DMA((EXCHANGES, sides)),
                pltpu.SemaphoreType.DMA((RESTARTS,)),
                pltpu.SemaphoreType.DMA((RESTARTS,)),
            ],
            compiler_params=pltpu.CompilerParams(
                collective_id=0, has_side_effects=True, vmem_limit_bytes=20 << 20
            ),
        )(step, *[pltpu.with_memory_space_constraint(x, pltpu.HBM) for x in (columns.T, lengths, lists[0], c, r, values)])

    placed = (
        P("dom", None),
        P("dom", None),
        P(),
        P("dom", None, None, None),
        P("dom", None),
        P("dom"),
        P("dom", None, None),
    )
    return jax.shard_map(
        shards, mesh=mesh, in_specs=placed, out_specs=P("dom", None), check_vma=False
    )
```

```python
import functools

import jax
import jax.numpy as jnp
from jax import lax
from jax.experimental import pallas as pl
from jax.experimental.pallas import tpu as pltpu
from jax.sharding import PartitionSpec as P

KRYLOV = 3
RESTARTS = 2
OFFSETS = (-2, -1, 1, 2)
SHIFT = 8.0
SCALE = 4.0
TILE = 8
EXCHANGES = 7
UP = 2
epsilon = 1e-06


def total(terms):
    result = terms[0]
    for term in terms[1:]:
        result = result + term
    return result


def quadratic(left, gram, right):
    return total(
        [a * total([gram[i][j] * b for j, b in enumerate(right)]) for i, a in enumerate(left)]
    )


def mapped_coefficients(c):
    result = [-SHIFT * c[0]]
    for i in range(1, len(c)):
        result.append(SCALE * c[i - 1] - SHIFT * c[i])
    result.append(SCALE * c[-1])
    return result


def subtract(a, weight, b):
    return [x - weight * b[i] if i < len(b) else x for i, x in enumerate(a)]


def multiply(a, b):
    size = len(a)
    result = []
    for i in range(size):
        row = []
        for j in range(size):
            terms = [
                a[i][k] * b[k][j]
                for k in range(size)
                if a[i][k] is not None and b[k][j] is not None
            ]
            row.append(total(terms) if terms else None)
        result.append(row)
    return result


def plus_identity(a, weight):
    return [
        [x * weight + 1.0 if i == j else x * weight for j, x in enumerate(row)]
        for i, row in enumerate(a)
    ]


def phi_column(hessenberg, substep):
    size = len(hessenberg)
    x = [
        [None if h is None else substep * h * (1.0 / 64.0) for h in row] for row in hessenberg
    ]
    one = jnp.ones_like(substep)
    zero = jnp.zeros_like(substep)
    series = [[one if i == j else zero for j in range(size)] for i in range(size)]
    for degree in range(12, 1, -1):
        series = plus_identity(multiply(x, series), 1.0 / degree)
    column = [series[i][0] * (1.0 / 64.0) for i in range(size)]
    power = plus_identity(multiply(x, series), 1.0)
    for turn in range(6):
        column = [
            total([power[i][k] * column[k] for k in range(size)]) + column[i] for i in range(size)
        ]
        if turn < 5:
            power = multiply(power, power)
    return column


def restart_coefficients(gram, substep):
    magnitude = jnp.sqrt(gram[0][0] + epsilon)
    basis = [[1.0 / magnitude]]
    hessenberg = [[None] * KRYLOV for _ in range(KRYLOV)]
    for column in range(KRYLOV):
        mapped = mapped_coefficients(basis[column])
        residue = mapped
        for k in range(column + 1):
            projection = quadratic(basis[k], gram, mapped)
            hessenberg[k][column] = projection
            residue = subtract(residue, projection, basis[k])
        if column + 1 < KRYLOV:
            squared = jnp.maximum(quadratic(residue, gram, residue), 0.0)
            length = jnp.sqrt(squared + epsilon)
            hessenberg[column + 1][column] = length
            inverse = 1.0 / length
            basis.append([x * inverse for x in residue])
    weights = phi_column(hessenberg, substep)
    factor = substep * magnitude
    return [
        factor * total([weights[k] * basis[k][i] for k in range(i, KRYLOV)]) for i in range(KRYLOV)
    ]


def merge_rows(parts):
    sublane = lax.broadcasted_iota(jnp.int32, parts[0].shape, 0)
    distance = 1
    while len(parts) > 1:
        first = (sublane // distance) % 2 == 0
        parts = [
            jnp.where(first, u, v)
            + pltpu.roll(jnp.where(first, v, u), TILE - distance, 0)
            for u, v in zip(parts[0::2], parts[1::2])
        ]
        distance *= 2
    return parts[0]


def kernel(n, *refs):
    operands, a_ref, y = refs[:6], refs[6], refs[7]
    staged = refs[8:14]
    step_ref, columns_ref, lengths_ref, lists_ref, c_ref, r_ref = staged
    scratch = list(refs[14:])
    stage_sem, inverse, order, table, places, a, local, rates, mixed = scratch[:9]
    columns_v, lengths_v, natural, z, w, w_send, w_recv = scratch[9:16]
    scratch = scratch[16:]
    extended = scratch[:EXCHANGES]
    packets = scratch[EXCHANGES : 2 * EXCHANGES]
    rest = scratch[2 * EXCHANGES :]
    sums, partial = rest[:RESTARTS], rest[RESTARTS : 2 * RESTARTS]
    load_sem, send_sem, recv_sem, sum_send, sum_recv = rest[2 * RESTARTS :]

    bdev, width = c_ref.shape
    slots = columns_ref.shape[0]
    sides, gmax = lists_ref.shape
    blank = bdev + sides * gmax
    me = lax.axis_index("dom")

    barrier = pltpu.get_barrier_semaphore()

    def greet(d, carry):
        pl.semaphore_signal(
            barrier,
            inc=1,
            device_id=(lax.rem(me + d, n),),
            device_id_type=pl.DeviceIdType.MESH,
        )
        return carry

    stages = [
        pltpu.make_async_copy(source, target, stage_sem.at[i])
        for i, (source, target) in enumerate(
            [*zip(operands, staged), (operands[1], columns_v), (operands[2], lengths_v)]
        )
    ]
    for copy in stages:
        copy.start()
    lax.fori_loop(1, n, greet, 0)
    loads = []
    for g in range(0, bdev, TILE):
        rows = pl.ds(g, TILE)
        copy = pltpu.make_async_copy(a_ref.at[rows], a.at[rows], load_sem.at[g // TILE])
        copy.start()
        loads.append(copy)
    for copy in stages:
        copy.wait()

    lead = (sides - 1) * lax.div(2 * me, n)

    def side(j):
        q = lax.rem(lead + j, sides)
        return q, q - 2 + lax.div(q, 2)

    def remote(e, q, offset, slot, source):
        return pltpu.make_async_remote_copy(
            src_ref=source,
            dst_ref=extended[e].at[pl.ds(bdev + q * gmax, gmax)],
            send_sem=send_sem.at[e, slot],
            recv_sem=recv_sem.at[e, q],
            device_id=(lax.rem(me + offset + n, n),),
            device_id_type=pl.DeviceIdType.MESH,
        )

    def first_copies():
        return [
            remote(0, q, offset, q, packets[0].at[q]) for q, offset in enumerate(OFFSETS)
        ]

    def copy_of(e, j):
        q, offset = side(j)
        source = packets[e].at[j] if j else extended[e].at[pl.ds(0, gmax)]
        return remote(e, q, offset, j, source)

    def send_lead(e):
        copy_of(e, 0).start()

    def pack(e, j, q):
        for g in range(gmax):
            packets[e][j, g : g + 1, :] = local[pl.ds(places[q * gmax + g], 1), :]

    def last_copies():
        return [
            remote(EXCHANGES - 1, q, OFFSETS[q], q, packets[EXCHANGES - 1].at[q])
            for q in range(UP, sides)
        ]

    def send_last():
        for q in range(UP, sides):
            pack(EXCHANGES - 1, q, q)
        for copy in last_copies():
            copy.start()
        for q in range(UP):
            pack(EXCHANGES - 1, q, q)

    def z_copies(i):
        return [
            pltpu.make_async_remote_copy(
                src_ref=z.at[i, pl.ds(bdev + q * gmax, gmax)],
                dst_ref=w.at[i, q],
                send_sem=w_send.at[i, q],
                recv_sem=w_recv.at[i, q],
                device_id=(lax.rem(me - OFFSETS[q] + n, n),),
                device_id_type=pl.DeviceIdType.MESH,
            )
            for q in range(UP)
        ]

    def send_rest(e):
        for j in range(1, sides):
            pack(e, j, side(j)[0])
        for j in range(1, sides):
            copy_of(e, j).start()

    def arrive(e):
        for q in range(sides):
            remote(e, q, 0, q, extended[e].at[pl.ds(0, gmax)]).wait_recv()

    def clear(target):
        target[blank:, :] = jnp.zeros((8, width), jnp.float32)

    for q in range(sides):
        for g in range(gmax):
            packets[0][q, g : g + 1, :] = c_ref[pl.ds(lists_ref[q, g], 1), :]
    pl.semaphore_wait(barrier, n - 1)
    for copy in first_copies():
        copy.start()

    def fill_inverse(row, carry):
        hit = jnp.int32(0)
        below = jnp.int32(0)
        for i in range(gmax):
            listed = lists_ref[lead, i]
            hit = jnp.where(listed == row, i + 1, hit)
            below = below + jnp.where(listed < row, 1, 0)
        inverse[row] = jnp.where(hit > 0, hit - 1, gmax + row - below)
        return carry

    lax.fori_loop(0, bdev, fill_inverse, 0)

    def fill_lead(i, carry):
        order[i] = lists_ref[lead, i]
        for q in range(sides):
            places[q * gmax + i] = inverse[lists_ref[q, i]]
        return carry

    lax.fori_loop(0, gmax, fill_lead, 0)

    def fill_others(i, carry):
        row = jnp.int32(0)
        for r in range(bdev):
            row = row + jnp.where(inverse[r] == i, r, 0)
        order[i] = row
        return carry

    lax.fori_loop(gmax, bdev, fill_others, 0)

    def fill_table(i, carry):
        row = order[i]
        length = lengths_ref[0, row]
        for t in range(1, slots):
            column = columns_ref[t, row]
            place = jnp.where(column < bdev, inverse[jnp.minimum(column, bdev - 1)], column)
            table[i * slots + t] = jnp.where(t < length, place, blank)
        return carry

    lax.fori_loop(0, bdev, fill_table, 0)

    def rowsum(products):
        turned = products.T
        return total([turned[k : k + TILE, :] for k in range(0, width, TILE)])

    def own_product(x):
        result = []
        for g in range(0, bdev, TILE):
            result.append(
                merge_rows(
                    [rowsum(a[order[i], 0] * x[i : i + 1, :]) for i in range(g, g + TILE)]
                )
            )
        return jnp.concatenate(result, axis=0)

    def other_product(source, start, stop):
        result = []
        for g in range(start, stop, TILE):
            parts = []
            for i in range(g, g + TILE):
                row = order[i]
                parts.append(
                    rowsum(
                        total(
                            [
                                a[row, t] * source[pl.ds(table[i * slots + t], 1), :]
                                for t in range(1, slots)
                            ]
                        )
                    )
                )
            result.append(merge_rows(parts))
        return jnp.concatenate(result, axis=0)

    lane = lax.broadcasted_iota(jnp.int32, (1, width), 1)

    def to_natural(k, field):
        local[...] = field
        for r in range(bdev):
            natural[k, r : r + 1, :] = local[pl.ds(inverse[r], 1), :]

    def one_hot():
        block = lax.broadcasted_iota(jnp.int32, (blank, bdev), 0)
        pieces = [
            jnp.where(
                (block == columns_v[t : t + 1, :]) & (lengths_v[...] > t), 1.0, 0.0
            )
            for t in range(1, slots)
        ]
        return jnp.concatenate(pieces, axis=1).astype(jnp.bfloat16)

    def transposed_product(i):
        sums = [[] for _ in range(slots)]
        for g in range(0, bdev, TILE):
            parts = [[] for _ in range(slots)]
            for r in range(g, g + TILE):
                turned = jnp.broadcast_to(natural[i, r : r + 1, :], (width, width)).T
                for t in range(slots):
                    parts[t].append(
                        total(
                            [
                                a[r, t, k : k + TILE, :] * turned[k : k + TILE, :]
                                for k in range(0, width, TILE)
                            ]
                        )
                    )
            for t in range(slots):
                sums[t].append(merge_rows(parts[t]))
        others = jnp.concatenate([p for t in range(1, slots) for p in sums[t]], axis=0)
        high = others.astype(jnp.bfloat16)
        low = (others - high.astype(jnp.float32)).astype(jnp.bfloat16)
        hot = one_hot()
        spread = total(
            [
                lax.dot_general(
                    hot,
                    half,
                    (((1,), (0,)), ((), ())),
                    preferred_element_type=jnp.float32,
                )
                for half in (high, low)
            ]
        )
        z[i, 0:bdev, :] = spread[0:bdev] + jnp.concatenate(sums[0], axis=0)
        z[i, bdev:, :] = spread[bdev:]
        for copy in z_copies(i):
            copy.start()

    def closing_dots(row, fields):
        e = EXCHANGES - 1
        last = len(fields)
        for i, field in enumerate(fields):
            terms = [
                (shifted * field) * fields[-1],
                z[i, 0:bdev, :] * natural[last - 1] * (-1.0 / SCALE),
            ]
            sums = [total([t[k : k + TILE] for k in range(0, bdev, TILE)]) for t in terms]
            pieces = [z[i, bdev + q * gmax : bdev + (q + 1) * gmax, :] * extended[e][
                bdev + q * gmax : bdev + (q + 1) * gmax, :
            ] for q in range(UP, sides)] + [w[i, q] * packets[e][q] for q in range(UP)]
            other = total([p[k : k + TILE] for p in pieces for k in range(0, gmax, TILE)])
            folded = total(sums) - other * (1.0 / SCALE)
            folded = jnp.sum(folded, axis=0, keepdims=True)
            value = jnp.sum(folded, axis=1, keepdims=True)
            row = jnp.where(lane == last * (last + 1) // 2 + i, value, row)
        return row

    def dots(row, fields, last):
        for i in range(last + 1):
            folded = jnp.sum(fields[i] * fields[last], axis=0, keepdims=True)
            value = jnp.sum(folded, axis=1, keepdims=True)
            row = jnp.where(lane == last * (last + 1) // 2 + i, value, row)
        return row

    def send_sums(turn, row):
        partial[turn][...] = row
        sums[turn][me] = row

        def one(d, carry):
            pltpu.make_async_remote_copy(
                src_ref=partial[turn],
                dst_ref=sums[turn].at[me],
                send_sem=sum_send.at[turn],
                recv_sem=sum_recv.at[turn],
                device_id=(lax.rem(me + d, n),),
                device_id_type=pl.DeviceIdType.MESH,
            ).start()
            return carry

        lax.fori_loop(1, n, one, 0)

    def gather_sums(turn, count):
        others = sums[turn].at[pl.ds(0, n - 1)]
        pltpu.make_async_copy(others, others, sum_recv.at[turn]).wait()
        row = jnp.sum(sums[turn][...], axis=0)
        gram = [[None] * count for _ in range(count)]
        for j in range(count):
            for i in range(j + 1):
                index = j * (j + 1) // 2 + i
                value = jnp.sum(jnp.where(lane == index, row, 0.0), axis=1, keepdims=True)
                gram[i][j] = gram[j][i] = jnp.broadcast_to(value, (8, width))
        return gram

    def combine(weights, fields):
        return total(
            [
                jnp.concatenate([w] * (f.shape[0] // 8), axis=0) * f
                for w, f in zip(weights, fields)
            ]
        )

    for i in range(bdev):
        row = order[i]
        local[i : i + 1, :] = c_ref[pl.ds(row, 1), :]
        rates[i : i + 1, :] = r_ref[pl.ds(row, 1), :]
    concentration = local[...]
    rate = rates[...]
    shifted = (rate * (1.0 - 2.0 * concentration) + SHIFT) * (1.0 / SCALE)
    substep = jnp.full((8, width), step_ref[0] * (1.0 / RESTARTS), jnp.float32)
    for e in range(EXCHANGES):
        clear(extended[e])
    clear(mixed)

    def finish(e, source, known, scale):
        parts = []
        for start in range(0, bdev, gmax):
            rows = slice(start, start + gmax)
            part = known[rows] - scale * other_product(source, start, start + gmax)
            parts.append(part)
            extended[e][rows, :] = part
            local[rows, :] = part
            if start == 0 and e < EXCHANGES - 1:
                send_lead(e)
        if e < EXCHANGES - 1:
            send_rest(e)
        else:
            send_last()
        return jnp.concatenate(parts, axis=0)

    def known_part(field):
        return shifted * field - own_product(field) * (1.0 / SCALE)

    extended[0][0:bdev, :] = concentration
    for copy in loads:
        copy.wait()
    known = rate * concentration * (1.0 - concentration) - own_product(concentration)
    arrive(0)
    field = finish(1, extended[0], known, 1.0)

    fields = [field]
    row = jnp.zeros((1, width), jnp.float32)
    for j in range(KRYLOV):
        row = dots(row, fields, j)
        known = known_part(field)
        arrive(1 + j)
        field = finish(2 + j, extended[1 + j], known, 1.0 / SCALE)
        fields.append(field)

    e = KRYLOV + 1
    send_sums(0, dots(row, fields, KRYLOV))
    known = known_part(field)
    arrive(e)
    field = finish(e + 1, extended[e], known, 1.0 / SCALE)
    fields.append(field)
    e = KRYLOV + 2
    d = restart_coefficients(gather_sums(0, KRYLOV + 1), substep)
    s = mapped_coefficients(d)
    s[0] = s[0] + 1.0
    start = combine(s, fields[:-1])
    field = combine(s, fields[1:])
    base = concentration + combine(d, fields[:KRYLOV])
    mixed[0:bdev, :] = field
    known = known_part(field)
    fields = [start, field]
    row = jnp.zeros((1, width), jnp.float32)
    row = dots(dots(row, fields, 0), fields, 1)
    to_natural(KRYLOV, base)
    for i, known_field in enumerate(fields):
        to_natural(i, known_field)
        transposed_product(i)
    arrive(e)
    mixed[bdev:blank, :] = combine(
        s, [extended[2 + j][bdev:blank, :] for j in range(KRYLOV + 1)]
    )
    field = finish(EXCHANGES - 1, mixed, known, 1.0 / SCALE)
    fields.append(field)
    to_natural(KRYLOV - 1, field)
    transposed_product(KRYLOV - 1)
    row = dots(row, fields, KRYLOV - 1)
    for q in range(UP, sides):
        remote(EXCHANGES - 1, q, 0, q, packets[EXCHANGES - 1].at[q]).wait_recv()
    for i in range(KRYLOV):
        for copy in z_copies(i):
            copy.wait_recv()
    send_sums(1, closing_dots(row, fields))
    d = restart_coefficients(gather_sums(1, KRYLOV + 1), substep)
    y[...] = natural[KRYLOV] + combine(d, [natural[i] for i in range(KRYLOV)])

    for copy in first_copies():
        copy.wait_send()
    for e in range(1, EXCHANGES - 1):
        for j in range(sides):
            copy_of(e, j).wait_send()
    for copy in last_copies() + [c for i in range(KRYLOV) for c in z_copies(i)]:
        copy.wait_send()
    for turn in range(RESTARTS):
        others = sums[turn].at[pl.ds(0, n - 1)]
        pltpu.make_async_copy(others, others, sum_send.at[turn]).wait()


def solution(mesh):
    n = mesh.shape["dom"]

    def shards(c, r, step, values, columns, lengths, lists):
        bdev, width = c.shape
        slots = columns.shape[1]
        sides, gmax = lists.shape[1:]
        tall = bdev + sides * gmax + 8
        f32 = jnp.float32
        held = pl.BlockSpec(memory_space=pltpu.HBM)
        vmem = pl.BlockSpec(memory_space=pltpu.VMEM)
        return pl.pallas_call(
            functools.partial(kernel, n),
            out_shape=jax.ShapeDtypeStruct((bdev, width), f32),
            in_specs=[held] * 7,
            out_specs=vmem,
            scratch_shapes=[
                pltpu.SMEM((1,), f32),
                pltpu.SMEM((slots, bdev), jnp.int32),
                pltpu.SMEM((1, bdev), jnp.int32),
                pltpu.SMEM((sides, gmax), jnp.int32),
                pltpu.VMEM((bdev, width), f32),
                pltpu.VMEM((bdev, width), f32),
                pltpu.SemaphoreType.DMA((8,)),
                pltpu.SMEM((bdev,), jnp.int32),
                pltpu.SMEM((bdev,), jnp.int32),
                pltpu.SMEM((bdev * slots,), jnp.int32),
                pltpu.SMEM((sides * gmax,), jnp.int32),
                pltpu.VMEM((bdev, slots, width, width), f32),
                pltpu.VMEM((bdev, width), f32),
                pltpu.VMEM((bdev, width), f32),
                pltpu.VMEM((tall, width), f32),
                pltpu.VMEM((slots, bdev), jnp.int32),
                pltpu.VMEM((1, bdev), jnp.int32),
                pltpu.VMEM((KRYLOV + 1, bdev, width), f32),
                pltpu.VMEM((KRYLOV, tall - 8, width), f32),
                pltpu.VMEM((KRYLOV, UP, gmax, width), f32),
                pltpu.SemaphoreType.DMA((KRYLOV, UP)),
                pltpu.SemaphoreType.DMA((KRYLOV, UP)),
            ]
            + [pltpu.VMEM((tall, width), f32)] * EXCHANGES
            + [pltpu.VMEM((sides, gmax, width), f32)] * EXCHANGES
            + [pltpu.VMEM((n, 1, width), f32)] * RESTARTS
            + [pltpu.VMEM((1, width), f32)] * RESTARTS
            + [
                pltpu.SemaphoreType.DMA((bdev // TILE,)),
                pltpu.SemaphoreType.DMA((EXCHANGES, sides)),
                pltpu.SemaphoreType.DMA((EXCHANGES, sides)),
                pltpu.SemaphoreType.DMA((RESTARTS,)),
                pltpu.SemaphoreType.DMA((RESTARTS,)),
            ],
            compiler_params=pltpu.CompilerParams(
                collective_id=0, has_side_effects=True, vmem_limit_bytes=24 << 20
            ),
        )(
            step,
            *[
                pltpu.with_memory_space_constraint(x, pltpu.HBM)
                for x in (columns.T, lengths.reshape(1, -1), lists[0], c, r, values)
            ],
        )

    placed = (
        P("dom", None),
        P("dom", None),
        P(),
        P("dom", None, None, None),
        P("dom", None),
        P("dom"),
        P("dom", None, None),
    )
    return jax.shard_map(
        shards, mesh=mesh, in_specs=placed, out_specs=P("dom", None), check_vma=False
    )
```

```python
import functools

import jax
import jax.numpy as jnp
from jax import lax
from jax.experimental import pallas as pl
from jax.experimental.pallas import tpu as pltpu
from jax.sharding import PartitionSpec as P

KRYLOV = 3
RESTARTS = 2
OFFSETS = (-2, -1, 1, 2)
SHIFT = 8.0
SCALE = 4.0
TILE = 8
EXCHANGES = 7
UP = 2
epsilon = 1e-06


def total(terms):
    result = terms[0]
    for term in terms[1:]:
        result = result + term
    return result


def quadratic(left, gram, right):
    return total(
        [a * total([gram[i][j] * b for j, b in enumerate(right)]) for i, a in enumerate(left)]
    )


def mapped_coefficients(c):
    result = [-SHIFT * c[0]]
    for i in range(1, len(c)):
        result.append(SCALE * c[i - 1] - SHIFT * c[i])
    result.append(SCALE * c[-1])
    return result


def subtract(a, weight, b):
    return [x - weight * b[i] if i < len(b) else x for i, x in enumerate(a)]


def multiply(a, b):
    size = len(a)
    result = []
    for i in range(size):
        row = []
        for j in range(size):
            terms = [
                a[i][k] * b[k][j]
                for k in range(size)
                if a[i][k] is not None and b[k][j] is not None
            ]
            row.append(total(terms) if terms else None)
        result.append(row)
    return result


def plus_identity(a, weight):
    return [
        [x * weight + 1.0 if i == j else x * weight for j, x in enumerate(row)]
        for i, row in enumerate(a)
    ]


def phi_column(hessenberg, substep):
    size = len(hessenberg)
    x = [
        [None if h is None else substep * h * (1.0 / 64.0) for h in row] for row in hessenberg
    ]
    one = jnp.ones_like(substep)
    zero = jnp.zeros_like(substep)
    series = [[one if i == j else zero for j in range(size)] for i in range(size)]
    for degree in range(12, 1, -1):
        series = plus_identity(multiply(x, series), 1.0 / degree)
    column = [series[i][0] * (1.0 / 64.0) for i in range(size)]
    power = plus_identity(multiply(x, series), 1.0)
    for turn in range(6):
        column = [
            total([power[i][k] * column[k] for k in range(size)]) + column[i] for i in range(size)
        ]
        if turn < 5:
            power = multiply(power, power)
    return column


def restart_coefficients(gram, substep):
    magnitude = jnp.sqrt(gram[0][0] + epsilon)
    basis = [[1.0 / magnitude]]
    hessenberg = [[None] * KRYLOV for _ in range(KRYLOV)]
    for column in range(KRYLOV):
        mapped = mapped_coefficients(basis[column])
        residue = mapped
        for k in range(column + 1):
            projection = quadratic(basis[k], gram, mapped)
            hessenberg[k][column] = projection
            residue = subtract(residue, projection, basis[k])
        if column + 1 < KRYLOV:
            squared = jnp.maximum(quadratic(residue, gram, residue), 0.0)
            length = jnp.sqrt(squared + epsilon)
            hessenberg[column + 1][column] = length
            inverse = 1.0 / length
            basis.append([x * inverse for x in residue])
    weights = phi_column(hessenberg, substep)
    factor = substep * magnitude
    return [
        factor * total([weights[k] * basis[k][i] for k in range(i, KRYLOV)]) for i in range(KRYLOV)
    ]


def merge_rows(parts):
    sublane = lax.broadcasted_iota(jnp.int32, parts[0].shape, 0)
    distance = 1
    while len(parts) > 1:
        first = (sublane // distance) % 2 == 0
        parts = [
            jnp.where(first, u, v)
            + pltpu.roll(jnp.where(first, v, u), TILE - distance, 0)
            for u, v in zip(parts[0::2], parts[1::2])
        ]
        distance *= 2
    return parts[0]


def kernel(n, *refs):
    operands, a_ref, y = refs[:6], refs[6], refs[7]
    staged = refs[8:14]
    step_ref, columns_ref, lengths_ref, lists_ref, c_ref, r_ref = staged
    scratch = list(refs[14:])
    stage_sem, inverse, order, table, places, a, local, rates, mixed = scratch[:9]
    columns_v, lengths_v, natural, z, w, closing, w_send, w_recv = scratch[9:17]
    scratch = scratch[17:]
    extended = scratch[:EXCHANGES]
    packets = scratch[EXCHANGES : 2 * EXCHANGES]
    rest = scratch[2 * EXCHANGES :]
    sums, partial = rest[:RESTARTS], rest[RESTARTS : 2 * RESTARTS]
    load_sem, send_sem, recv_sem, sum_send, sum_recv = rest[2 * RESTARTS :]

    bdev, width = c_ref.shape
    slots = columns_ref.shape[0]
    sides, gmax = lists_ref.shape
    blank = bdev + sides * gmax
    me = lax.axis_index("dom")

    barrier = pltpu.get_barrier_semaphore()

    def greet(d, carry):
        pl.semaphore_signal(
            barrier,
            inc=1,
            device_id=(lax.rem(me + d, n),),
            device_id_type=pl.DeviceIdType.MESH,
        )
        return carry

    stages = [
        pltpu.make_async_copy(source, target, stage_sem.at[i])
        for i, (source, target) in enumerate(
            [*zip(operands, staged), (operands[1], columns_v), (operands[2], lengths_v)]
        )
    ]
    for copy in stages:
        copy.start()
    lax.fori_loop(1, n, greet, 0)
    loads = []
    for g in range(0, bdev, TILE):
        rows = pl.ds(g, TILE)
        copy = pltpu.make_async_copy(a_ref.at[rows], a.at[rows], load_sem.at[g // TILE])
        copy.start()
        loads.append(copy)
    for copy in stages:
        copy.wait()

    lead = (sides - 1) * lax.div(2 * me, n)

    def side(j):
        q = lax.rem(lead + j, sides)
        return q, q - 2 + lax.div(q, 2)

    def remote(e, q, offset, slot, source):
        return pltpu.make_async_remote_copy(
            src_ref=source,
            dst_ref=extended[e].at[pl.ds(bdev + q * gmax, gmax)],
            send_sem=send_sem.at[e, slot],
            recv_sem=recv_sem.at[e, q],
            device_id=(lax.rem(me + offset + n, n),),
            device_id_type=pl.DeviceIdType.MESH,
        )

    def first_copies():
        return [
            remote(0, q, offset, q, packets[0].at[q]) for q, offset in enumerate(OFFSETS)
        ]

    def copy_of(e, j):
        q, offset = side(j)
        source = packets[e].at[j] if j else extended[e].at[pl.ds(0, gmax)]
        return remote(e, q, offset, j, source)

    def send_lead(e):
        copy_of(e, 0).start()

    def pack(e, j, q):
        for g in range(gmax):
            packets[e][j, g : g + 1, :] = local[pl.ds(places[q * gmax + g], 1), :]

    def last_copy(q):
        return remote(EXCHANGES - 1, q, OFFSETS[q], q, packets[EXCHANGES - 1].at[q])

    def z_copy(i, q):
        return pltpu.make_async_remote_copy(
            src_ref=z.at[i, pl.ds(bdev + q * gmax, gmax)],
            dst_ref=w.at[i, q],
            send_sem=w_send.at[i, q],
            recv_sem=w_recv.at[i, q],
            device_id=(lax.rem(me - OFFSETS[q] + n, n),),
            device_id_type=pl.DeviceIdType.MESH,
        )

    def at_the_bottom(q):
        return me + OFFSETS[q] < 0

    def at_the_top(q):
        return me - OFFSETS[q] >= n

    def send_last():
        for q in range(sides):
            pack(EXCHANGES - 1, q, q)
        for q in range(UP, sides):
            last_copy(q).start()
        for q in range(UP):

            @pl.when(jnp.logical_not(at_the_bottom(q)))
            def _():
                last_copy(q).start()

    def send_rest(e):
        for j in range(1, sides):
            pack(e, j, side(j)[0])
        for j in range(1, sides):
            copy_of(e, j).start()

    def arrive(e):
        for q in range(sides):
            remote(e, q, 0, q, extended[e].at[pl.ds(0, gmax)]).wait_recv()

    def clear(target):
        target[blank:, :] = jnp.zeros((8, width), jnp.float32)

    for q in range(sides):
        for g in range(gmax):
            packets[0][q, g : g + 1, :] = c_ref[pl.ds(lists_ref[q, g], 1), :]
    def fill_inverse(row, carry):
        hit = jnp.int32(0)
        below = jnp.int32(0)
        for i in range(gmax):
            listed = lists_ref[lead, i]
            hit = jnp.where(listed == row, i + 1, hit)
            below = below + jnp.where(listed < row, 1, 0)
        inverse[row] = jnp.where(hit > 0, hit - 1, gmax + row - below)
        return carry

    def fill_lead(i, carry):
        order[i] = lists_ref[lead, i]
        for q in range(sides):
            places[q * gmax + i] = inverse[lists_ref[q, i]]
        return carry

    def fill_others(i, carry):
        row = jnp.int32(0)
        for r in range(bdev):
            row = row + jnp.where(inverse[r] == i, r, 0)
        order[i] = row
        return carry

    def fill_table(i, carry):
        row = order[i]
        length = lengths_ref[0, row]
        for t in range(1, slots):
            column = columns_ref[t, row]
            place = jnp.where(column < bdev, inverse[jnp.minimum(column, bdev - 1)], column)
            table[i * slots + t] = jnp.where(t < length, place, blank)
        return carry

    def tables():
        lax.fori_loop(0, bdev, fill_inverse, 0)
        lax.fori_loop(0, gmax, fill_lead, 0)
        lax.fori_loop(gmax, bdev, fill_others, 0)
        lax.fori_loop(0, bdev, fill_table, 0)

    @pl.when(2 * me < n)
    def _():
        tables()

    pl.semaphore_wait(barrier, n - 1)
    for copy in first_copies():
        copy.start()

    @pl.when(2 * me >= n)
    def _():
        tables()

    def rowsum(products):
        turned = products.T
        return total([turned[k : k + TILE, :] for k in range(0, width, TILE)])

    def own_product(x):
        result = []
        for g in range(0, bdev, TILE):
            result.append(
                merge_rows(
                    [rowsum(a[order[i], 0] * x[i : i + 1, :]) for i in range(g, g + TILE)]
                )
            )
        return jnp.concatenate(result, axis=0)

    def other_product(source, start, stop):
        result = []
        for g in range(start, stop, TILE):
            parts = []
            for i in range(g, g + TILE):
                row = order[i]
                parts.append(
                    rowsum(
                        total(
                            [
                                a[row, t] * source[pl.ds(table[i * slots + t], 1), :]
                                for t in range(1, slots)
                            ]
                        )
                    )
                )
            result.append(merge_rows(parts))
        return jnp.concatenate(result, axis=0)

    lane = lax.broadcasted_iota(jnp.int32, (1, width), 1)

    def to_natural(k, field):
        local[...] = field
        for r in range(bdev):
            natural[k, r : r + 1, :] = local[pl.ds(inverse[r], 1), :]

    def one_hot():
        block = lax.broadcasted_iota(jnp.int32, (blank, bdev), 0)
        pieces = [
            jnp.where(
                (block == columns_v[t : t + 1, :]) & (lengths_v[...] > t), 1.0, 0.0
            )
            for t in range(1, slots)
        ]
        return jnp.concatenate(pieces, axis=1).astype(jnp.bfloat16)

    def transposed_product(i):
        sums = [[] for _ in range(slots)]
        for g in range(0, bdev, TILE):
            parts = [[] for _ in range(slots)]
            for r in range(g, g + TILE):
                turned = jnp.broadcast_to(natural[i, r : r + 1, :], (width, width)).T
                for t in range(slots):
                    parts[t].append(
                        total(
                            [
                                a[r, t, k : k + TILE, :] * turned[k : k + TILE, :]
                                for k in range(0, width, TILE)
                            ]
                        )
                    )
            for t in range(slots):
                sums[t].append(merge_rows(parts[t]))
        others = jnp.concatenate([p for t in range(1, slots) for p in sums[t]], axis=0)
        high = others.astype(jnp.bfloat16)
        low = (others - high.astype(jnp.float32)).astype(jnp.bfloat16)
        hot = one_hot()
        spread = total(
            [
                lax.dot_general(
                    hot,
                    half,
                    (((1,), (0,)), ((), ())),
                    preferred_element_type=jnp.float32,
                )
                for half in (high, low)
            ]
        )
        z[i, 0:bdev, :] = spread[0:bdev] + jnp.concatenate(sums[0], axis=0)
        z[i, bdev:, :] = spread[bdev:]
        for q in range(UP):

            @pl.when(at_the_top(q))
            def _():
                z_copy(i, q).start()

    def fold(field):
        return total([field[k : k + TILE] for k in range(0, field.shape[0], TILE)])

    def closing_dots(row, fields):
        e = EXCHANGES - 1
        last = len(fields)
        minus = -1.0 / SCALE

        def ghosts(i, q):
            rows = slice(bdev + q * gmax, bdev + (q + 1) * gmax)
            return fold(z[i, rows, :] * extended[e][rows, :])

        def arrived(q):
            remote(e, q, 0, q, packets[e].at[q]).wait_recv()

        for i, field in enumerate(fields):
            own = fold(z[i, 0:bdev, :] * natural[last - 1])
            closing[i] = fold((shifted * field) * fields[-1]) + own * minus
        for q in range(UP):

            @pl.when(at_the_bottom(q))
            def _():
                for i in range(last):
                    z_copy(i, q).wait_recv()
                    closing[i] = closing[i] + fold(w[i, q] * packets[e][q]) * minus

            @pl.when(jnp.logical_not(at_the_top(q)))
            def _():
                arrived(q)
                for i in range(last):
                    closing[i] = closing[i] + ghosts(i, q) * minus

        for q in range(UP, sides):
            arrived(q)
        for i in range(last):
            folded = closing[i] + total([ghosts(i, q) for q in range(UP, sides)]) * minus
            folded = jnp.sum(folded, axis=0, keepdims=True)
            value = jnp.sum(folded, axis=1, keepdims=True)
            row = jnp.where(lane == last * (last + 1) // 2 + i, value, row)
        return row

    def dots(row, fields, last):
        for i in range(last + 1):
            folded = jnp.sum(fields[i] * fields[last], axis=0, keepdims=True)
            value = jnp.sum(folded, axis=1, keepdims=True)
            row = jnp.where(lane == last * (last + 1) // 2 + i, value, row)
        return row

    def send_sums(turn, row):
        partial[turn][...] = row
        sums[turn][me] = row

        def one(d, carry):
            pltpu.make_async_remote_copy(
                src_ref=partial[turn],
                dst_ref=sums[turn].at[me],
                send_sem=sum_send.at[turn],
                recv_sem=sum_recv.at[turn],
                device_id=(lax.rem(me + d, n),),
                device_id_type=pl.DeviceIdType.MESH,
            ).start()
            return carry

        lax.fori_loop(1, n, one, 0)

    def gather_sums(turn, count):
        others = sums[turn].at[pl.ds(0, n - 1)]
        pltpu.make_async_copy(others, others, sum_recv.at[turn]).wait()
        row = jnp.sum(sums[turn][...], axis=0)
        gram = [[None] * count for _ in range(count)]
        for j in range(count):
            for i in range(j + 1):
                index = j * (j + 1) // 2 + i
                value = jnp.sum(jnp.where(lane == index, row, 0.0), axis=1, keepdims=True)
                gram[i][j] = gram[j][i] = jnp.broadcast_to(value, (8, width))
        return gram

    def combine(weights, fields):
        return total(
            [
                jnp.concatenate([w] * (f.shape[0] // 8), axis=0) * f
                for w, f in zip(weights, fields)
            ]
        )

    for i in range(bdev):
        row = order[i]
        local[i : i + 1, :] = c_ref[pl.ds(row, 1), :]
        rates[i : i + 1, :] = r_ref[pl.ds(row, 1), :]
    concentration = local[...]
    rate = rates[...]
    shifted = (rate * (1.0 - 2.0 * concentration) + SHIFT) * (1.0 / SCALE)
    substep = jnp.full((8, width), step_ref[0] * (1.0 / RESTARTS), jnp.float32)
    for e in range(EXCHANGES):
        clear(extended[e])
    clear(mixed)

    def finish(e, source, known, scale):
        parts = []
        for start in range(0, bdev, gmax):
            rows = slice(start, start + gmax)
            part = known[rows] - scale * other_product(source, start, start + gmax)
            parts.append(part)
            extended[e][rows, :] = part
            local[rows, :] = part
            if start == 0 and e < EXCHANGES - 1:
                send_lead(e)
        if e < EXCHANGES - 1:
            send_rest(e)
        else:
            send_last()
        return jnp.concatenate(parts, axis=0)

    def known_part(field):
        return shifted * field - own_product(field) * (1.0 / SCALE)

    extended[0][0:bdev, :] = concentration
    for copy in loads:
        copy.wait()
    known = rate * concentration * (1.0 - concentration) - own_product(concentration)
    arrive(0)
    field = finish(1, extended[0], known, 1.0)

    fields = [field]
    row = jnp.zeros((1, width), jnp.float32)
    for j in range(KRYLOV):
        row = dots(row, fields, j)
        known = known_part(field)
        arrive(1 + j)
        field = finish(2 + j, extended[1 + j], known, 1.0 / SCALE)
        fields.append(field)

    e = KRYLOV + 1
    send_sums(0, dots(row, fields, KRYLOV))
    known = known_part(field)
    arrive(e)
    field = finish(e + 1, extended[e], known, 1.0 / SCALE)
    fields.append(field)
    e = KRYLOV + 2
    d = restart_coefficients(gather_sums(0, KRYLOV + 1), substep)
    s = mapped_coefficients(d)
    s[0] = s[0] + 1.0
    start = combine(s, fields[:-1])
    field = combine(s, fields[1:])
    base = concentration + combine(d, fields[:KRYLOV])
    mixed[0:bdev, :] = field
    known = known_part(field)
    fields = [start, field]
    row = jnp.zeros((1, width), jnp.float32)
    row = dots(dots(row, fields, 0), fields, 1)
    to_natural(KRYLOV, base)
    for i, known_field in enumerate(fields):
        to_natural(i, known_field)
        transposed_product(i)
    arrive(e)
    mixed[bdev:blank, :] = combine(
        s, [extended[2 + j][bdev:blank, :] for j in range(KRYLOV + 1)]
    )
    field = finish(EXCHANGES - 1, mixed, known, 1.0 / SCALE)
    fields.append(field)
    to_natural(KRYLOV - 1, field)
    transposed_product(KRYLOV - 1)
    row = dots(row, fields, KRYLOV - 1)
    send_sums(1, closing_dots(row, fields))
    d = restart_coefficients(gather_sums(1, KRYLOV + 1), substep)
    y[...] = natural[KRYLOV] + combine(d, [natural[i] for i in range(KRYLOV)])

    for copy in first_copies():
        copy.wait_send()
    for e in range(1, EXCHANGES - 1):
        for j in range(sides):
            copy_of(e, j).wait_send()
    for q in range(UP, sides):
        last_copy(q).wait_send()
    for q in range(UP):

        @pl.when(jnp.logical_not(at_the_bottom(q)))
        def _():
            last_copy(q).wait_send()

        @pl.when(at_the_top(q))
        def _():
            for i in range(KRYLOV):
                z_copy(i, q).wait_send()

    for turn in range(RESTARTS):
        others = sums[turn].at[pl.ds(0, n - 1)]
        pltpu.make_async_copy(others, others, sum_send.at[turn]).wait()


def solution(mesh):
    n = mesh.shape["dom"]

    def shards(c, r, step, values, columns, lengths, lists):
        bdev, width = c.shape
        slots = columns.shape[1]
        sides, gmax = lists.shape[1:]
        tall = bdev + sides * gmax + 8
        f32 = jnp.float32
        held = pl.BlockSpec(memory_space=pltpu.HBM)
        vmem = pl.BlockSpec(memory_space=pltpu.VMEM)
        return pl.pallas_call(
            functools.partial(kernel, n),
            out_shape=jax.ShapeDtypeStruct((bdev, width), f32),
            in_specs=[held] * 7,
            out_specs=vmem,
            scratch_shapes=[
                pltpu.SMEM((1,), f32),
                pltpu.SMEM((slots, bdev), jnp.int32),
                pltpu.SMEM((1, bdev), jnp.int32),
                pltpu.SMEM((sides, gmax), jnp.int32),
                pltpu.VMEM((bdev, width), f32),
                pltpu.VMEM((bdev, width), f32),
                pltpu.SemaphoreType.DMA((8,)),
                pltpu.SMEM((bdev,), jnp.int32),
                pltpu.SMEM((bdev,), jnp.int32),
                pltpu.SMEM((bdev * slots,), jnp.int32),
                pltpu.SMEM((sides * gmax,), jnp.int32),
                pltpu.VMEM((bdev, slots, width, width), f32),
                pltpu.VMEM((bdev, width), f32),
                pltpu.VMEM((bdev, width), f32),
                pltpu.VMEM((tall, width), f32),
                pltpu.VMEM((slots, bdev), jnp.int32),
                pltpu.VMEM((1, bdev), jnp.int32),
                pltpu.VMEM((KRYLOV + 1, bdev, width), f32),
                pltpu.VMEM((KRYLOV, tall - 8, width), f32),
                pltpu.VMEM((KRYLOV, UP, gmax, width), f32),
                pltpu.VMEM((KRYLOV, TILE, width), f32),
                pltpu.SemaphoreType.DMA((KRYLOV, UP)),
                pltpu.SemaphoreType.DMA((KRYLOV, UP)),
            ]
            + [pltpu.VMEM((tall, width), f32)] * EXCHANGES
            + [pltpu.VMEM((sides, gmax, width), f32)] * EXCHANGES
            + [pltpu.VMEM((n, 1, width), f32)] * RESTARTS
            + [pltpu.VMEM((1, width), f32)] * RESTARTS
            + [
                pltpu.SemaphoreType.DMA((bdev // TILE,)),
                pltpu.SemaphoreType.DMA((EXCHANGES, sides)),
                pltpu.SemaphoreType.DMA((EXCHANGES, sides)),
                pltpu.SemaphoreType.DMA((RESTARTS,)),
                pltpu.SemaphoreType.DMA((RESTARTS,)),
            ],
            compiler_params=pltpu.CompilerParams(
                collective_id=0, has_side_effects=True, vmem_limit_bytes=24 << 20
            ),
        )(
            step,
            *[
                pltpu.with_memory_space_constraint(x, pltpu.HBM)
                for x in (columns.T, lengths.reshape(1, -1), lists[0], c, r, values)
            ],
        )

    placed = (
        P("dom", None),
        P("dom", None),
        P(),
        P("dom", None, None, None),
        P("dom", None),
        P("dom"),
        P("dom", None, None),
    )
    return jax.shard_map(
        shards, mesh=mesh, in_specs=placed, out_specs=P("dom", None), check_vma=False
    )
```

```python
import functools

import jax
import jax.numpy as jnp
from jax import lax
from jax.experimental import pallas as pl
from jax.experimental.pallas import tpu as pltpu
from jax.sharding import PartitionSpec as P

KRYLOV = 3
RESTARTS = 2
OFFSETS = (-2, -1, 1, 2)
SHIFT = 8.0
SCALE = 4.0
TILE = 8
EXCHANGES = 7
UP = 2
epsilon = 1e-06


def total(terms):
    result = terms[0]
    for term in terms[1:]:
        result = result + term
    return result


def quadratic(left, gram, right):
    return total(
        [a * total([gram[i][j] * b for j, b in enumerate(right)]) for i, a in enumerate(left)]
    )


def mapped_coefficients(c):
    result = [-SHIFT * c[0]]
    for i in range(1, len(c)):
        result.append(SCALE * c[i - 1] - SHIFT * c[i])
    result.append(SCALE * c[-1])
    return result


def subtract(a, weight, b):
    return [x - weight * b[i] if i < len(b) else x for i, x in enumerate(a)]


def multiply(a, b):
    size = len(a)
    result = []
    for i in range(size):
        row = []
        for j in range(size):
            terms = [
                a[i][k] * b[k][j]
                for k in range(size)
                if a[i][k] is not None and b[k][j] is not None
            ]
            row.append(total(terms) if terms else None)
        result.append(row)
    return result


def plus_identity(a, weight):
    return [
        [x * weight + 1.0 if i == j else x * weight for j, x in enumerate(row)]
        for i, row in enumerate(a)
    ]


def phi_column(hessenberg, substep):
    size = len(hessenberg)
    x = [
        [None if h is None else substep * h * (1.0 / 64.0) for h in row] for row in hessenberg
    ]
    one = jnp.ones_like(substep)
    zero = jnp.zeros_like(substep)
    series = [[one if i == j else zero for j in range(size)] for i in range(size)]
    for degree in range(12, 1, -1):
        series = plus_identity(multiply(x, series), 1.0 / degree)
    column = [series[i][0] * (1.0 / 64.0) for i in range(size)]
    power = plus_identity(multiply(x, series), 1.0)
    for turn in range(6):
        column = [
            total([power[i][k] * column[k] for k in range(size)]) + column[i] for i in range(size)
        ]
        if turn < 5:
            power = multiply(power, power)
    return column


def restart_coefficients(gram, substep):
    magnitude = jnp.sqrt(gram[0][0] + epsilon)
    basis = [[1.0 / magnitude]]
    hessenberg = [[None] * KRYLOV for _ in range(KRYLOV)]
    for column in range(KRYLOV):
        mapped = mapped_coefficients(basis[column])
        residue = mapped
        for k in range(column + 1):
            projection = quadratic(basis[k], gram, mapped)
            hessenberg[k][column] = projection
            residue = subtract(residue, projection, basis[k])
        if column + 1 < KRYLOV:
            squared = jnp.maximum(quadratic(residue, gram, residue), 0.0)
            length = jnp.sqrt(squared + epsilon)
            hessenberg[column + 1][column] = length
            inverse = 1.0 / length
            basis.append([x * inverse for x in residue])
    weights = phi_column(hessenberg, substep)
    factor = substep * magnitude
    return [
        factor * total([weights[k] * basis[k][i] for k in range(i, KRYLOV)]) for i in range(KRYLOV)
    ]


def merge_rows(parts):
    sublane = lax.broadcasted_iota(jnp.int32, parts[0].shape, 0)
    distance = 1
    while len(parts) > 1:
        first = (sublane // distance) % 2 == 0
        parts = [
            jnp.where(first, u, v)
            + pltpu.roll(jnp.where(first, v, u), TILE - distance, 0)
            for u, v in zip(parts[0::2], parts[1::2])
        ]
        distance *= 2
    return parts[0]


def kernel(n, *refs):
    operands, a_ref, y = refs[:6], refs[6], refs[7]
    staged = refs[8:14]
    step_ref, columns_ref, lengths_ref, lists_ref, c_ref, r_ref = staged
    scratch = list(refs[14:])
    stage_sem, inverse, order, table, places, a, local, rates, mixed = scratch[:9]
    columns_v, lengths_v, natural, z, w, closing, w_send, w_recv = scratch[9:17]
    relay, relay_send, relay_recv, back, ahead, spread_sem = scratch[17:23]
    scratch = scratch[23:]
    extended = scratch[:EXCHANGES]
    packets = scratch[EXCHANGES : 2 * EXCHANGES]
    rest = scratch[2 * EXCHANGES :]
    sums, partial = rest[:RESTARTS], rest[RESTARTS : 2 * RESTARTS]
    load_sem, send_sem, recv_sem, sum_send, sum_recv = rest[2 * RESTARTS :]

    bdev, width = c_ref.shape
    slots = columns_ref.shape[0]
    sides, gmax = lists_ref.shape
    blank = bdev + sides * gmax
    me = lax.axis_index("dom")

    barrier = pltpu.get_barrier_semaphore()

    odd = lax.rem(me, 2) == 1
    even = jnp.logical_not(odd)

    def signal(semaphore, d):
        pl.semaphore_signal(
            semaphore,
            inc=1,
            device_id=(lax.rem(me + d + n, n),),
            device_id_type=pl.DeviceIdType.MESH,
        )

    signal(barrier, -2)

    @pl.when(even)
    def _():
        signal(barrier, 1)
        signal(barrier, -1)

    @pl.when(me == 1)
    def _():
        signal(barrier, -3)

    stages = [
        pltpu.make_async_copy(source, target, stage_sem.at[i])
        for i, (source, target) in enumerate(
            [*zip(operands, staged), (operands[1], columns_v), (operands[2], lengths_v)]
        )
    ]
    for copy in stages:
        copy.start()
    @pl.when(odd)
    def _():
        pl.semaphore_wait(barrier, 3)
        signal(back.at[0], 2)
        signal(back.at[2], -1)

        @pl.when(me != n - 1)
        def _():
            signal(back.at[1], 1)

    @pl.when(even)
    def _():
        pl.semaphore_wait(barrier, 1 + (me == n - 2).astype(jnp.int32))

        @pl.when(me != n - 2)
        def _():
            signal(back.at[0], 2)

        @pl.when(me == n - 2)
        def _():
            signal(ahead.at[0], 3)

    for copy in stages:
        copy.wait()
    loads = []
    for g in range(0, bdev, TILE):
        rows = pl.ds(g, TILE)
        copy = pltpu.make_async_copy(a_ref.at[rows], a.at[rows], load_sem.at[g // TILE])
        copy.start()
        loads.append(copy)

    lead = (sides - 1) * lax.div(2 * me, n)

    def side(j):
        q = lax.rem(lead + j, sides)
        return q, q - 2 + lax.div(q, 2)

    def remote(e, q, offset, slot, source):
        return pltpu.make_async_remote_copy(
            src_ref=source,
            dst_ref=extended[e].at[pl.ds(bdev + q * gmax, gmax)],
            send_sem=send_sem.at[e, slot],
            recv_sem=recv_sem.at[e, q],
            device_id=(lax.rem(me + offset + n, n),),
            device_id_type=pl.DeviceIdType.MESH,
        )

    def first_copy(q):
        return remote(0, q, OFFSETS[q], q, packets[0].at[q])

    def relay_in(q):
        return pltpu.make_async_remote_copy(
            src_ref=packets[0].at[q],
            dst_ref=relay.at[q],
            send_sem=send_sem.at[0, q],
            recv_sem=relay_recv.at[q],
            device_id=(lax.rem(me + 1, n),),
            device_id_type=pl.DeviceIdType.MESH,
        )

    def relay_out(q):
        return pltpu.make_async_remote_copy(
            src_ref=relay.at[q],
            dst_ref=extended[0].at[pl.ds(bdev + q * gmax, gmax)],
            send_sem=relay_send.at[q],
            recv_sem=recv_sem.at[0, q],
            device_id=(lax.rem(me - 1 + OFFSETS[q] + n, n),),
            device_id_type=pl.DeviceIdType.MESH,
        )

    def copy_of(e, j):
        q, offset = side(j)
        source = packets[e].at[j] if j else extended[e].at[pl.ds(0, gmax)]
        return remote(e, q, offset, j, source)

    def send_lead(e):
        copy_of(e, 0).start()

    def pack(e, j, q):
        for g in range(gmax):
            packets[e][j, g : g + 1, :] = local[pl.ds(places[q * gmax + g], 1), :]

    def last_copy(q):
        return remote(EXCHANGES - 1, q, OFFSETS[q], q, packets[EXCHANGES - 1].at[q])

    def z_copy(i, q):
        return pltpu.make_async_remote_copy(
            src_ref=z.at[i, pl.ds(bdev + q * gmax, gmax)],
            dst_ref=w.at[i, q],
            send_sem=w_send.at[i, q],
            recv_sem=w_recv.at[i, q],
            device_id=(lax.rem(me - OFFSETS[q] + n, n),),
            device_id_type=pl.DeviceIdType.MESH,
        )

    def at_the_bottom(q):
        return me + OFFSETS[q] < 0

    def at_the_top(q):
        return me - OFFSETS[q] >= n

    def send_last():
        for q in range(sides):
            pack(EXCHANGES - 1, q, q)
        for q in range(UP, sides):
            last_copy(q).start()
        for q in range(UP):

            @pl.when(jnp.logical_not(at_the_bottom(q)))
            def _():
                last_copy(q).start()

    def send_rest(e):
        for j in range(1, sides):
            pack(e, j, side(j)[0])
        for j in range(1, sides):
            copy_of(e, j).start()

    def arrive(e):
        for q in range(sides):
            remote(e, q, 0, q, extended[e].at[pl.ds(0, gmax)]).wait_recv()

    def clear(target):
        target[blank:, :] = jnp.zeros((8, width), jnp.float32)

    for q in range(sides):
        for g in range(gmax):
            packets[0][q, g : g + 1, :] = c_ref[pl.ds(lists_ref[q, g], 1), :]
    def fill_inverse(row, carry):
        hit = jnp.int32(0)
        below = jnp.int32(0)
        for i in range(gmax):
            listed = lists_ref[lead, i]
            hit = jnp.where(listed == row, i + 1, hit)
            below = below + jnp.where(listed < row, 1, 0)
        inverse[row] = jnp.where(hit > 0, hit - 1, gmax + row - below)
        return carry

    def fill_lead(i, carry):
        order[i] = lists_ref[lead, i]
        for q in range(sides):
            places[q * gmax + i] = inverse[lists_ref[q, i]]
        return carry

    def fill_others(i, carry):
        row = jnp.int32(0)
        for r in range(bdev):
            row = row + jnp.where(inverse[r] == i, r, 0)
        order[i] = row
        return carry

    def fill_table(i, carry):
        row = order[i]
        length = lengths_ref[0, row]
        for t in range(1, slots):
            column = columns_ref[t, row]
            place = jnp.where(column < bdev, inverse[jnp.minimum(column, bdev - 1)], column)
            table[i * slots + t] = jnp.where(t < length, place, blank)
        return carry

    def tables():
        lax.fori_loop(0, bdev, fill_inverse, 0)
        lax.fori_loop(0, gmax, fill_lead, 0)
        lax.fori_loop(gmax, bdev, fill_others, 0)
        lax.fori_loop(0, bdev, fill_table, 0)

    @pl.when(me < 2)
    def _():
        tables()


    @pl.when(odd)
    def _():
        first_copy(3).start()
        first_copy(1).start()
        first_copy(2).start()
        pl.semaphore_wait(back.at[0], 1)
        first_copy(0).start()

    @pl.when(even)
    def _():
        first_copy(3).start()
        pl.semaphore_wait(back.at[2], 1)
        first_copy(2).start()

        @pl.when(me == 0)
        def _():
            for q in range(UP):
                relay_in(q).start()

        @pl.when(me != 0)
        def _():
            pl.semaphore_wait(back.at[1], 1)
            first_copy(1).start()
            pl.semaphore_wait(back.at[0], 1)
            first_copy(0).start()

    @pl.when(me == 1)
    def _():
        for q in range(UP):
            relay_in(q).wait_recv()
        pl.semaphore_wait(ahead.at[0], 1)
        for q in range(UP):
            relay_out(q).start()

    @pl.when(me >= 2)
    def _():
        tables()

    def rowsum(products):
        turned = products.T
        return total([turned[k : k + TILE, :] for k in range(0, width, TILE)])

    def own_product(x):
        result = []
        for g in range(0, bdev, TILE):
            result.append(
                merge_rows(
                    [rowsum(a[order[i], 0] * x[i : i + 1, :]) for i in range(g, g + TILE)]
                )
            )
        return jnp.concatenate(result, axis=0)

    def other_product(source, start, stop):
        result = []
        for g in range(start, stop, TILE):
            parts = []
            for i in range(g, g + TILE):
                row = order[i]
                parts.append(
                    rowsum(
                        total(
                            [
                                a[row, t] * source[pl.ds(table[i * slots + t], 1), :]
                                for t in range(1, slots)
                            ]
                        )
                    )
                )
            result.append(merge_rows(parts))
        return jnp.concatenate(result, axis=0)

    lane = lax.broadcasted_iota(jnp.int32, (1, width), 1)

    def to_natural(k, field):
        local[...] = field
        for r in range(bdev):
            natural[k, r : r + 1, :] = local[pl.ds(inverse[r], 1), :]

    def one_hot():
        block = lax.broadcasted_iota(jnp.int32, (blank, bdev), 0)
        pieces = [
            jnp.where(
                (block == columns_v[t : t + 1, :]) & (lengths_v[...] > t), 1.0, 0.0
            )
            for t in range(1, slots)
        ]
        return jnp.concatenate(pieces, axis=1).astype(jnp.bfloat16)

    def transposed_product(i):
        sums = [[] for _ in range(slots)]
        for g in range(0, bdev, TILE):
            parts = [[] for _ in range(slots)]
            for r in range(g, g + TILE):
                turned = jnp.broadcast_to(natural[i, r : r + 1, :], (width, width)).T
                for t in range(slots):
                    parts[t].append(
                        total(
                            [
                                a[r, t, k : k + TILE, :] * turned[k : k + TILE, :]
                                for k in range(0, width, TILE)
                            ]
                        )
                    )
            for t in range(slots):
                sums[t].append(merge_rows(parts[t]))
        others = jnp.concatenate([p for t in range(1, slots) for p in sums[t]], axis=0)
        high = others.astype(jnp.bfloat16)
        low = (others - high.astype(jnp.float32)).astype(jnp.bfloat16)
        hot = one_hot()
        spread = total(
            [
                lax.dot_general(
                    hot,
                    half,
                    (((1,), (0,)), ((), ())),
                    preferred_element_type=jnp.float32,
                )
                for half in (high, low)
            ]
        )
        z[i, 0:bdev, :] = spread[0:bdev] + jnp.concatenate(sums[0], axis=0)
        z[i, bdev:, :] = spread[bdev:]
        for q in range(UP):

            @pl.when(at_the_top(q))
            def _():
                z_copy(i, q).start()

    def fold(field):
        return total([field[k : k + TILE] for k in range(0, field.shape[0], TILE)])

    def closing_dots(row, fields):
        e = EXCHANGES - 1
        last = len(fields)
        minus = -1.0 / SCALE

        def ghosts(i, q):
            rows = slice(bdev + q * gmax, bdev + (q + 1) * gmax)
            return fold(z[i, rows, :] * extended[e][rows, :])

        def arrived(q):
            remote(e, q, 0, q, packets[e].at[q]).wait_recv()

        for i, field in enumerate(fields):
            own = fold(z[i, 0:bdev, :] * natural[last - 1])
            closing[i] = fold((shifted * field) * fields[-1]) + own * minus
        for q in range(UP):

            @pl.when(at_the_bottom(q))
            def _():
                for i in range(last):
                    z_copy(i, q).wait_recv()
                    closing[i] = closing[i] + fold(w[i, q] * packets[e][q]) * minus

            @pl.when(jnp.logical_not(at_the_top(q)))
            def _():
                arrived(q)
                for i in range(last):
                    closing[i] = closing[i] + ghosts(i, q) * minus

        for q in range(UP, sides):
            arrived(q)
        for i in range(last):
            folded = closing[i] + total([ghosts(i, q) for q in range(UP, sides)]) * minus
            folded = jnp.sum(folded, axis=0, keepdims=True)
            value = jnp.sum(folded, axis=1, keepdims=True)
            row = jnp.where(lane == last * (last + 1) // 2 + i, value, row)
        return row

    def dots(row, fields, last):
        for i in range(last + 1):
            folded = jnp.sum(fields[i] * fields[last], axis=0, keepdims=True)
            value = jnp.sum(folded, axis=1, keepdims=True)
            row = jnp.where(lane == last * (last + 1) // 2 + i, value, row)
        return row

    def send_sums(turn, row):
        partial[turn][...] = row
        sums[turn][me] = row

        def one(d, carry):
            pltpu.make_async_remote_copy(
                src_ref=partial[turn],
                dst_ref=sums[turn].at[me],
                send_sem=sum_send.at[turn],
                recv_sem=sum_recv.at[turn],
                device_id=(lax.rem(me + d, n),),
                device_id_type=pl.DeviceIdType.MESH,
            ).start()
            return carry

        lax.fori_loop(1, n, one, 0)

    def gather_sums(turn, count):
        others = sums[turn].at[pl.ds(0, n - 1)]
        pltpu.make_async_copy(others, others, sum_recv.at[turn]).wait()
        row = jnp.sum(sums[turn][...], axis=0)
        gram = [[None] * count for _ in range(count)]
        for j in range(count):
            for i in range(j + 1):
                index = j * (j + 1) // 2 + i
                value = jnp.sum(jnp.where(lane == index, row, 0.0), axis=1, keepdims=True)
                gram[i][j] = gram[j][i] = jnp.broadcast_to(value, (8, width))
        return gram

    def combine(weights, fields):
        return total(
            [
                jnp.concatenate([w] * (f.shape[0] // 8), axis=0) * f
                for w, f in zip(weights, fields)
            ]
        )

    for i in range(bdev):
        row = order[i]
        local[i : i + 1, :] = c_ref[pl.ds(row, 1), :]
        rates[i : i + 1, :] = r_ref[pl.ds(row, 1), :]
    concentration = local[...]
    rate = rates[...]
    shifted = (rate * (1.0 - 2.0 * concentration) + SHIFT) * (1.0 / SCALE)
    substep = jnp.full((8, width), step_ref[0] * (1.0 / RESTARTS), jnp.float32)
    for e in range(EXCHANGES):
        clear(extended[e])
    clear(mixed)

    def finish(e, source, known, scale):
        parts = []
        for start in range(0, bdev, gmax):
            rows = slice(start, start + gmax)
            part = known[rows] - scale * other_product(source, start, start + gmax)
            parts.append(part)
            extended[e][rows, :] = part
            local[rows, :] = part
            if start == 0 and e < EXCHANGES - 1:
                send_lead(e)
        if e < EXCHANGES - 1:
            send_rest(e)
        else:
            send_last()
        return jnp.concatenate(parts, axis=0)

    def known_part(field):
        return shifted * field - own_product(field) * (1.0 / SCALE)

    extended[0][0:bdev, :] = concentration
    for copy in loads:
        copy.wait()
    known = rate * concentration * (1.0 - concentration) - own_product(concentration)
    arrive(0)
    field = finish(1, extended[0], known, 1.0)

    reaches = [2]
    while 4 * reaches[-1] < n:
        reaches.append(2 * reaches[-1])

    def heard(k):
        pl.semaphore_wait(spread_sem.at[k], 2)

    def spread(start, stop):
        for k in range(start, min(stop, len(reaches))):
            if k:
                heard(k - 1)
            signal(spread_sem.at[k], reaches[k])
            signal(spread_sem.at[k], -reaches[k])

    share = -(-len(reaches) // KRYLOV)
    fields = [field]
    row = jnp.zeros((1, width), jnp.float32)
    for j in range(KRYLOV):
        spread(j * share, (j + 1) * share)
        row = dots(row, fields, j)
        known = known_part(field)
        arrive(1 + j)
        field = finish(2 + j, extended[1 + j], known, 1.0 / SCALE)
        fields.append(field)

    e = KRYLOV + 1
    heard(len(reaches) - 1)
    send_sums(0, dots(row, fields, KRYLOV))
    known = known_part(field)
    arrive(e)
    field = finish(e + 1, extended[e], known, 1.0 / SCALE)
    fields.append(field)
    e = KRYLOV + 2
    d = restart_coefficients(gather_sums(0, KRYLOV + 1), substep)
    s = mapped_coefficients(d)
    s[0] = s[0] + 1.0
    start = combine(s, fields[:-1])
    field = combine(s, fields[1:])
    base = concentration + combine(d, fields[:KRYLOV])
    mixed[0:bdev, :] = field
    known = known_part(field)
    fields = [start, field]
    row = jnp.zeros((1, width), jnp.float32)
    row = dots(dots(row, fields, 0), fields, 1)
    to_natural(KRYLOV, base)
    for i, known_field in enumerate(fields):
        to_natural(i, known_field)
        transposed_product(i)
    arrive(e)
    mixed[bdev:blank, :] = combine(
        s, [extended[2 + j][bdev:blank, :] for j in range(KRYLOV + 1)]
    )
    field = finish(EXCHANGES - 1, mixed, known, 1.0 / SCALE)
    fields.append(field)
    to_natural(KRYLOV - 1, field)
    transposed_product(KRYLOV - 1)
    row = dots(row, fields, KRYLOV - 1)
    send_sums(1, closing_dots(row, fields))
    d = restart_coefficients(gather_sums(1, KRYLOV + 1), substep)
    y[...] = natural[KRYLOV] + combine(d, [natural[i] for i in range(KRYLOV)])

    for q in range(sides):
        first_copy(q).wait_send()

    @pl.when(me == 1)
    def _():
        for q in range(UP):
            relay_out(q).wait_send()

    for e in range(1, EXCHANGES - 1):
        for j in range(sides):
            copy_of(e, j).wait_send()
    for q in range(UP, sides):
        last_copy(q).wait_send()
    for q in range(UP):

        @pl.when(jnp.logical_not(at_the_bottom(q)))
        def _():
            last_copy(q).wait_send()

        @pl.when(at_the_top(q))
        def _():
            for i in range(KRYLOV):
                z_copy(i, q).wait_send()

    for turn in range(RESTARTS):
        others = sums[turn].at[pl.ds(0, n - 1)]
        pltpu.make_async_copy(others, others, sum_send.at[turn]).wait()


def solution(mesh):
    n = mesh.shape["dom"]

    def shards(c, r, step, values, columns, lengths, lists):
        bdev, width = c.shape
        slots = columns.shape[1]
        sides, gmax = lists.shape[1:]
        tall = bdev + sides * gmax + 8
        f32 = jnp.float32
        held = pl.BlockSpec(memory_space=pltpu.HBM)
        vmem = pl.BlockSpec(memory_space=pltpu.VMEM)
        return pl.pallas_call(
            functools.partial(kernel, n),
            out_shape=jax.ShapeDtypeStruct((bdev, width), f32),
            in_specs=[held] * 7,
            out_specs=vmem,
            scratch_shapes=[
                pltpu.SMEM((1,), f32),
                pltpu.SMEM((slots, bdev), jnp.int32),
                pltpu.SMEM((1, bdev), jnp.int32),
                pltpu.SMEM((sides, gmax), jnp.int32),
                pltpu.VMEM((bdev, width), f32),
                pltpu.VMEM((bdev, width), f32),
                pltpu.SemaphoreType.DMA((8,)),
                pltpu.SMEM((bdev,), jnp.int32),
                pltpu.SMEM((bdev,), jnp.int32),
                pltpu.SMEM((bdev * slots,), jnp.int32),
                pltpu.SMEM((sides * gmax,), jnp.int32),
                pltpu.VMEM((bdev, slots, width, width), f32),
                pltpu.VMEM((bdev, width), f32),
                pltpu.VMEM((bdev, width), f32),
                pltpu.VMEM((tall, width), f32),
                pltpu.VMEM((slots, bdev), jnp.int32),
                pltpu.VMEM((1, bdev), jnp.int32),
                pltpu.VMEM((KRYLOV + 1, bdev, width), f32),
                pltpu.VMEM((KRYLOV, tall - 8, width), f32),
                pltpu.VMEM((KRYLOV, UP, gmax, width), f32),
                pltpu.VMEM((KRYLOV, TILE, width), f32),
                pltpu.SemaphoreType.DMA((KRYLOV, UP)),
                pltpu.SemaphoreType.DMA((KRYLOV, UP)),
                pltpu.VMEM((UP, gmax, width), f32),
                pltpu.SemaphoreType.DMA((UP,)),
                pltpu.SemaphoreType.DMA((UP,)),
                pltpu.SemaphoreType.REGULAR((UP + 1,)),
                pltpu.SemaphoreType.REGULAR((1,)),
                pltpu.SemaphoreType.REGULAR((n.bit_length(),)),
            ]
            + [pltpu.VMEM((tall, width), f32)] * EXCHANGES
            + [pltpu.VMEM((sides, gmax, width), f32)] * EXCHANGES
            + [pltpu.VMEM((n, 1, width), f32)] * RESTARTS
            + [pltpu.VMEM((1, width), f32)] * RESTARTS
            + [
                pltpu.SemaphoreType.DMA((bdev // TILE,)),
                pltpu.SemaphoreType.DMA((EXCHANGES, sides)),
                pltpu.SemaphoreType.DMA((EXCHANGES, sides)),
                pltpu.SemaphoreType.DMA((RESTARTS,)),
                pltpu.SemaphoreType.DMA((RESTARTS,)),
            ],
            compiler_params=pltpu.CompilerParams(
                collective_id=0, has_side_effects=True, vmem_limit_bytes=24 << 20
            ),
        )(
            step,
            *[
                pltpu.with_memory_space_constraint(x, pltpu.HBM)
                for x in (columns.T, lengths.reshape(1, -1), lists[0], c, r, values)
            ],
        )

    placed = (
        P("dom", None),
        P("dom", None),
        P(),
        P("dom", None, None, None),
        P("dom", None),
        P("dom"),
        P("dom", None, None),
    )
    return jax.shard_map(
        shards, mesh=mesh, in_specs=placed, out_specs=P("dom", None), check_vma=False
    )
```
